256 devices in a mesh: section: 16 (over y, z_lo), dp: 16 (over z_hi, x, core).
Axes of the slice: x: 4, y: 4, z: 8 (z_hi: 2, z_lo: 4; z = z_hi * 4 + z_lo), core: 2. Of those that a mesh axis runs over, the one named last changes fastest.
Arguments:
- vit_weight: bfloat16 [16, 1280, 1280], P('section', 'dp'), may hold values from -0.078125 to 0.078125
- t5_weight: bfloat16 [16, 2048, 2048], P('section', 'dp'), may hold values from -0.0625 to 0.0625
- vit_saved: bfloat16 [16, 4, 512, 1280], P('section', None, 'dp'), may hold values from -6 to 6
- t5_saved: bfloat16 [16, 4, 512, 2048], P('section', None, 'dp'), may hold values from -6 to 6
- vit_top_grad: bfloat16 [4, 512, 1280], P(None, 'dp'), may hold values from -6 to 6
- t5_top_grad: bfloat16 [4, 512, 2048], P(None, 'dp'), may hold values from -6 to 6
Outputs:
- vit_input_grads: bfloat16 [16, 4, 512, 1280], P('section', None, 'dp')
- t5_input_grads: bfloat16 [16, 4, 512, 2048], P('section', None, 'dp')
- vit_weight_grads: float32 [16, 1280, 1280], P('section', 'dp')
- t5_weight_grads: float32 [16, 2048, 2048], P('section', 'dp')
The draws below stay inside these ranges and needn't reach their ends.
All inputs are finite; a program needn't handle non-finite values.
Results may differ from the reference program's by a relative error of at most 0.02.
Values may be sent and summed in bfloat16 or wider, within the bound.
A program may use at most 128 MiB of HBM per device.

```python
import jax
import jax.numpy as jnp
from jax import lax

DV = 1280
DT = 2048
TOK = 32
MB = 4
LAYERS = 16
TOKENS = 512
N_DP = 16


def spiked(entries, own_key, source, target, blocks, factor):
    owner, partner = [(jnp.arange(entries.shape[axis_at]) // (entries.shape[axis_at] // blocks)).reshape([-1 if axis == axis_at else 1 for axis in range(entries.ndim)]) for axis_at in (source, target)]
    chosen = jax.random.permutation(own_key, blocks)[partner]
    strong = (owner == chosen) | (owner == (partner + blocks // 2) % blocks)
    return jnp.where(strong, factor * entries, entries)


def level_of(own_key, shape, pieces, low, high):
    def one(dim, blocks):
        heights = jax.random.uniform(jax.random.fold_in(jax.random.fold_in(own_key, 6), dim), (blocks,), jnp.float32, low / len(pieces), high / len(pieces))
        return jnp.repeat(jnp.exp(heights), shape[dim] // blocks).reshape((-1,) + (1,) * (len(shape) - dim - 1))

    loudness = one(*pieces[0])
    for cut in pieces[1:]:
        loudness = loudness * one(*cut)
    return loudness


def normal_values(rng, shape, width, most, split=(), kind=jnp.bfloat16):
    drawn = jax.random.normal(rng, shape, jnp.float32) * width
    if len(split) > 0:
        drawn = level_of(rng, shape, split, -0.22, 0.18) * drawn
    return jnp.clip(drawn, min=-most, max=most).astype(kind)


def gaussian_with(own_key, dims, scale, bound, split, heavy, dtype=jnp.bfloat16):
    values = scale * jax.random.normal(own_key, dims, jnp.float32)
    if split:
        values = values * level_of(own_key, dims, split, -0.22, 0.18)
    return jnp.clip(spiked(values, jax.random.fold_in(own_key, 3), *heavy), -bound, bound).astype(dtype)


def setup_inputs(seed: int = 0) -> dict:
    keys = jax.random.split(jax.random.key(seed), 7)
    return {
        "vit_weight": normal_values(keys[0], (LAYERS, DV, DV), (4 * DV) ** -0.5, 0.078125, ((0, 16), (1, 16))),
        "t5_weight": normal_values(keys[1], (LAYERS, DT, DT), (4 * DT) ** -0.5, 0.0625, ((0, 16), (1, 16))),
        "vit_saved": gaussian_with(keys[2], (LAYERS, MB, TOKENS, DV), 1.0, 6.0, ((0, 16), (2, 16)), (2, 3, 16, 2.0)),
        "t5_saved": gaussian_with(keys[3], (LAYERS, MB, TOKENS, DT), 1.0, 6.0, ((0, 16), (2, 16)), (2, 3, 16, 2.0)),
        "vit_top_grad": normal_values(keys[4], (MB, TOKENS, DV), 1.0, 6.0, ((1, 16),)),
        "t5_top_grad": normal_values(keys[5], (MB, TOKENS, DT), 1.0, 6.0, ((1, 16),)),
    }


root_half = 0.7071067811865476
inv_root_tau = 0.3989422804014327


def gelu_slope(preact):
    cumulative = 0.5 * (1.0 + lax.erf(preact * root_half))
    density = jnp.exp(-0.5 * preact * preact) * inv_root_tau
    return cumulative + preact * density


def layer_back(grad_above, saved_input, weight):
    preact = jnp.dot(saved_input, weight, preferred_element_type=jnp.float32)
    upper = grad_above.astype(jnp.float32)
    local_grad = (upper * gelu_slope(preact)).astype(jnp.bfloat16)
    through = jnp.dot(local_grad, weight.T, preferred_element_type=jnp.float32)
    return (upper + through).astype(jnp.bfloat16), local_grad


def run_branch(weights, saved, top_grad):
    layer_count = weights.shape[0]
    features = top_grad.shape[2]
    grad_above = top_grad.reshape(MB * TOKENS, features)
    input_grads = [None] * layer_count
    weight_grads = [None] * layer_count
    for layer_index in reversed(range(layer_count)):
        saved_input = saved[layer_index].reshape(MB * TOKENS, features)
        grad_below, local_grad = layer_back(grad_above, saved_input, weights[layer_index])
        grouped_input = saved_input.astype(jnp.float32).reshape(MB, N_DP, TOK, features)
        grouped_local = local_grad.astype(jnp.float32).reshape(MB, N_DP, TOK, features)
        partial_value = jnp.einsum("mpti,mptj->pij", grouped_input, grouped_local) * (1.0 / (MB * TOK))
        rounded = lax.optimization_barrier(partial_value.astype(jnp.bfloat16))
        weight_grads[layer_index] = jnp.sum(rounded.astype(jnp.float32), axis=0)
        input_grads[layer_index] = grad_below.reshape(MB, TOKENS, features)
        grad_above = grad_below
    return jnp.stack(input_grads), jnp.stack(weight_grads)


def reference(vit_weight, t5_weight, vit_saved, t5_saved, vit_top_grad, t5_top_grad):
    vit_grads, vit_wgrads = run_branch(vit_weight, vit_saved, vit_top_grad)
    t5_grads, t5_wgrads = run_branch(t5_weight, t5_saved, t5_top_grad)
    return (vit_grads, t5_grads, vit_wgrads, t5_wgrads)
```

```python
import jax
import jax.numpy as jnp
from jax import lax
from jax.experimental import pallas as pl
from jax.experimental.pallas import tpu as pltpu
from jax.sharding import PartitionSpec as P

MESH = pl.DeviceIdType.MESH
root_half = 0.7071067811865476
inv_root_tau = 0.3989422804014327

SECTIONS = 16
DP = 16
DV = 1280
DT = 2048
RV = DV // DP
RT = DT // DP
TOK = 128
MICRO = 16
MB = TOK // MICRO
CHUNKS = 4
CT = 512
EARLY = 9


def slope_of(preact):
    cumulative = 0.5 * (1.0 + lax.erf(preact * root_half))
    density = jnp.exp(-0.5 * preact * preact) * inv_root_tau
    return cumulative + preact * density


def nt(a, b):
    return lax.dot_general(a, b, (((1,), (1,)), ((), ())), preferred_element_type=jnp.float32)


def nn(a, b):
    return jnp.dot(a, b, preferred_element_type=jnp.float32)


def ds(start, size, unit):
    return pl.ds(pl.multiple_of(start, unit), size)


class Gather:
    def __init__(self, slot, part, recv, pair, sent):
        self.slot, self.part, self.recv, self.pair, self.sent = slot, part, recv, pair, sent


def kernel(
    w5, wv, s5, sv, s5t, svt, top5, topv,
    g5o, gvo, d5o, dvo,
    W5, WV, L5, LV, S5, SV, G5, GV, P5, PV,
    rw5, rwv, rl5, rlv, pair, sent, c5, cv, csent, asem, asent, lsem,
):
    s = lax.axis_index("section")
    d = lax.axis_index("dp")
    zh = lax.div(d, 8)
    x = lax.rem(lax.div(d, 2), 4)
    c = lax.rem(d, 2)
    dr = 1 - 2 * c

    def dev(half, step, core):
        return lax.rem(zh + half, 2) * 8 + lax.rem(x + step + 8, 4) * 2 + core

    nx = dev(0, dr, c)
    zp = dev(1, 0, c)
    pt = dev(0, 0, 1 - c)
    first = s == SECTIONS - 1
    lower = s > 0
    early = s < EARLY

    barrier = pltpu.get_barrier_semaphore()

    def greet(p, _):
        pl.semaphore_signal(
            barrier, inc=1, device_id=(s, lax.rem(d + p, DP)), device_id_type=MESH
        )
        return 0

    lax.fori_loop(1, DP, greet, 0)

    @pl.when(lower)
    def _():
        pl.semaphore_signal(barrier, inc=1, device_id=(s - 1, d), device_id_type=MESH)

    @pl.when(s < SECTIONS - 1)
    def _():
        pl.semaphore_signal(barrier, inc=1, device_id=(s + 1, d), device_id_type=MESH)

    sections = lax.div(s + SECTIONS - 1, SECTIONS) + lax.div(2 * SECTIONS - 2 - s, SECTIONS)
    pl.semaphore_wait(barrier, DP - 1 + sections)

    gw5 = Gather(
        lambda v, q: W5.at[ds(q * (DT // CHUNKS), DT // CHUNKS, 16), ds(v * RT, RT, RT)],
        lambda n: W5.at[:, pl.ds(0, n * RT)],
        rw5, pair.at[0], sent.at[0],
    )
    gwv = Gather(
        lambda v, q: WV.at[ds(v * RV, RV, 16), :],
        lambda n: WV.at[pl.ds(0, n * RV), :],
        rwv, pair.at[1], sent.at[1],
    )
    gl5 = Gather(
        lambda v, q: L5.at[ds(v * TOK + q * (TOK // CHUNKS), TOK // CHUNKS, 16), :],
        lambda n: L5.at[pl.ds(0, n * TOK), :],
        rl5, pair.at[2], sent.at[2],
    )
    glv = Gather(
        lambda v, q: LV.at[ds(v * TOK + q * (TOK // CHUNKS), TOK // CHUNKS, 16), :],
        lambda n: LV.at[pl.ds(0, n * TOK), :],
        rlv, pair.at[3], sent.at[3],
    )

    def push(g, owner, q, recv, to):
        return pltpu.make_async_remote_copy(
            src_ref=g.slot(owner, q), dst_ref=g.slot(owner, q), send_sem=g.sent, recv_sem=recv,
            device_id=(s, to), device_id_type=MESH,
        )

    def own_ring(g, q):
        push(g, d, q, g.recv.at[0, 1, q], nx).start()

    def own_far(g, q):
        push(g, d, q, g.recv.at[1, 0, q], zp).start()

    def own_pair(g, q):
        push(g, d, q, g.pair, pt).start()

    def own(g, q):
        own_ring(g, q)
        own_far(g, q)
        own_pair(g, q)

    def forward(g, h, r, q):
        owner = dev(h, -r * dr, c)
        push(g, owner, q, g.recv.at[h, r, q], nx).wait_recv()
        if r < 3:
            push(g, owner, q, g.recv.at[h, r + 1, q], nx).start()
        push(g, owner, q, g.pair, pt).start()

    def forward_when(g, h, r, q):
        @pl.when(jnp.logical_and(q >= 0, q < CHUNKS))
        def _():
            forward(g, h, r, q)

    def ring_phase(g, r):
        def one(q, _):
            forward(g, 0, r, q)
            return 0

        lax.fori_loop(0, CHUNKS, one, 0)

    def far_phase(g):
        def one(w, _):
            for r in range(4):
                forward_when(g, 1, r, w - r)
            return 0

        lax.fori_loop(0, CHUNKS + 3, one, 0)

    def pair_done(g):
        ref = g.part(DP // 2)
        pltpu.make_async_copy(ref, ref, g.pair).wait()

    def sent_done(g):
        ref = g.part(DP - 1)
        pltpu.make_async_copy(ref, ref, g.sent).wait()

    own_w5 = pltpu.make_async_copy(w5, W5.at[:, ds(d * RT, RT, RT)], lsem.at[0])
    own_wv = pltpu.make_async_copy(wv, WV.at[ds(d * RV, RV, 16), :], lsem.at[1])
    own_s5 = pltpu.make_async_copy(
        s5t.at[ds(d * RT, RT, RT), :], S5.at[:, ds(d * TOK, TOK, TOK)], lsem.at[2]
    )
    own_sv = pltpu.make_async_copy(
        svt.at[ds(d * RV, RV, 16), :], SV.at[:, ds(d * TOK, TOK, TOK)], lsem.at[3]
    )
    own_w5.start()
    own_wv.start()
    own_s5.start()
    own_sv.start()
    own_w5.wait()
    for q in range(CHUNKS):
        own(gw5, q)
    own_wv.wait()
    own_far(gwv, 0)

    @pl.when(first)
    def _():
        a = pltpu.make_async_copy(top5, G5, lsem.at[0])
        b = pltpu.make_async_copy(topv, GV, lsem.at[1])
        a.start()
        b.start()
        a.wait()
        b.wait()

    own_s5.wait()
    own_sv.wait()
    for r in (1, 2, 3):
        ring_phase(gw5, r)
    far_phase(gw5)
    own_ring(gwv, 0)
    own_pair(gwv, 0)
    pair_done(gw5)

    def text_slope(j, _):
        cols = ds(j * CT, CT, CT)
        P5[:, cols] = slope_of(nt(s5[...], W5[cols, :]))
        return 0

    lax.fori_loop(0, DT // CT, text_slope, 0)

    image_steps = ((1, 0), (0, 1), (1, 1), (0, 2), (1, 2), (0, 3), (1, 3))

    def image_ready():
        pair_done(gwv)

        def one(j, _):
            cols = ds(j * 256, 256, 256)
            PV[:, cols] = slope_of(nn(sv[...], WV[:, cols]))
            return 0

        lax.fori_loop(0, DV // 256, one, 0)

        def send(p, _):
            t = lax.rem(d + p, DP)
            pltpu.make_async_remote_copy(
                src_ref=s5t.at[ds(t * RT, RT, RT), :], dst_ref=S5.at[:, ds(d * TOK, TOK, TOK)],
                send_sem=asent.at[0], recv_sem=asem.at[0], device_id=(s, t), device_id_type=MESH,
            ).start()
            pltpu.make_async_remote_copy(
                src_ref=svt.at[ds(t * RV, RV, 16), :], dst_ref=SV.at[:, ds(d * TOK, TOK, TOK)],
                send_sem=asent.at[1], recv_sem=asem.at[1], device_id=(s, t), device_id_type=MESH,
            ).start()
            return 0

        lax.fori_loop(1, DP, send, 0)

    @pl.when(early)
    def _():
        for h, r in image_steps:
            forward(gwv, h, r, 0)
        image_ready()

    def text_hop(k, n):
        rows, cols = ds(k * MICRO, MICRO, MICRO), pl.ds(n * CT, CT)
        return pltpu.make_async_remote_copy(
            src_ref=g5o.at[rows, cols], dst_ref=G5.at[rows, cols], send_sem=csent.at[0], recv_sem=c5.at[k, n],
            device_id=(s - 1, d), device_id_type=MESH,
        )

    def text_tick(k, _):
        rows = ds(k * MICRO, MICRO, MICRO)

        @pl.when(jnp.logical_not(first))
        def _():
            for n in range(DT // CT):
                text_hop(k, n).wait_recv()

        upper = G5[rows, :].astype(jnp.float32)
        local = (upper * P5[rows, :]).astype(jnp.bfloat16)
        L5[ds(d * TOK + k * MICRO, MICRO, MICRO), :] = local
        for n in range(DT // CT):
            cols = pl.ds(n * CT, CT)
            above = G5[rows, cols].astype(jnp.float32)
            g5o[rows, cols] = (above + nn(local, W5[:, cols])).astype(jnp.bfloat16)

            @pl.when(lower)
            def _():
                text_hop(k, n).start()

        odd = lax.rem(k, 2) == 1

        @pl.when(odd)
        def _():
            own(gl5, lax.div(k, 2))

        @pl.when(jnp.logical_and(odd, k >= 3))
        def _():
            forward(gl5, 0, 1, lax.div(k, 2) - 1)

        @pl.when(jnp.logical_not(early))
        def _():
            for i, (h, r) in enumerate(image_steps):

                @pl.when(k == i)
                def _():
                    forward(gwv, h, r, 0)

        return 0

    lax.fori_loop(0, MB, text_tick, 0)

    @pl.when(jnp.logical_not(early))
    def _():
        image_ready()

    def image_hop(k):
        rows = ds(k * MICRO, MICRO, MICRO)
        return pltpu.make_async_remote_copy(
            src_ref=gvo.at[rows, :], dst_ref=GV.at[rows, :], send_sem=csent.at[1], recv_sem=cv.at[k],
            device_id=(s - 1, d), device_id_type=MESH,
        )

    def image_tick(k, _):
        rows = ds(k * MICRO, MICRO, MICRO)

        @pl.when(jnp.logical_not(first))
        def _():
            image_hop(k).wait_recv()

        upper = GV[rows, :].astype(jnp.float32)
        local = (upper * PV[rows, :]).astype(jnp.bfloat16)
        LV[ds(d * TOK + k * MICRO, MICRO, MICRO), :] = local
        gvo[rows, :] = (upper + nt(local, WV[...])).astype(jnp.bfloat16)

        @pl.when(lower)
        def _():
            image_hop(k).start()

        @pl.when(lax.rem(k, 2) == 1)
        def _():
            own(glv, lax.div(k, 2))

        @pl.when(k == 0)
        def _():
            forward(gl5, 0, 1, CHUNKS - 1)

        forward_when(gl5, 0, 2, k)
        forward_when(gl5, 0, 3, k - 1)
        for r in range(4):
            forward_when(gl5, 1, r, k - 1 - r)
        return 0

    lax.fori_loop(0, MB, image_tick, 0)
    ring_phase(glv, 1)
    ring_phase(glv, 2)
    pair_done(gl5)
    got = S5.at[:, pl.ds(0, (DP - 1) * TOK)]
    pltpu.make_async_copy(got, got, asem.at[0]).wait()

    def text_total(j, _):
        cols = ds(j * CT, CT, CT)
        d5o[:, cols] = nn(S5[...], L5[:, cols]) * (1.0 / TOK)
        return 0

    lax.fori_loop(0, DT // CT, text_total, 0)
    ring_phase(glv, 3)
    far_phase(glv)
    pair_done(glv)
    got = SV.at[:, pl.ds(0, (DP - 1) * TOK)]
    pltpu.make_async_copy(got, got, asem.at[1]).wait()

    def image_total(j, _):
        cols = ds(j * 256, 256, 256)
        dvo[:, cols] = nn(SV[...], LV[:, cols]) * (1.0 / TOK)
        return 0

    lax.fori_loop(0, DV // 256, image_total, 0)
    for g in (gw5, gwv, gl5, glv):
        sent_done(g)
    gone = s5t.at[pl.ds(0, (DP - 1) * RT), :]
    pltpu.make_async_copy(gone, gone, asent.at[0]).wait()
    gone = svt.at[pl.ds(0, (DP - 1) * RV), :]
    pltpu.make_async_copy(gone, gone, asent.at[1]).wait()

    @pl.when(lower)
    def _():
        pltpu.make_async_copy(g5o, g5o, csent.at[0]).wait()
        pltpu.make_async_copy(gvo, gvo, csent.at[1]).wait()


def shards(vit_weight, t5_weight, vit_saved, t5_saved, vit_top_grad, t5_top_grad):
    s5 = t5_saved.reshape(TOK, DT)
    sv = vit_saved.reshape(TOK, DV)
    bf, f32 = jnp.bfloat16, jnp.float32
    dma, vmem = pltpu.SemaphoreType.DMA, pl.BlockSpec(memory_space=pltpu.VMEM)
    g5, gv, d5, dv = pl.pallas_call(
        kernel,
        out_shape=(
            jax.ShapeDtypeStruct((TOK, DT), bf),
            jax.ShapeDtypeStruct((TOK, DV), bf),
            jax.ShapeDtypeStruct((RT, DT), f32),
            jax.ShapeDtypeStruct((RV, DV), f32),
        ),
        in_specs=[vmem] * 8,
        out_specs=[vmem] * 4,
        scratch_shapes=[
            pltpu.VMEM((DT, DT), bf),
            pltpu.VMEM((DV, DV), bf),
            pltpu.VMEM((DP * TOK, DT), bf),
            pltpu.VMEM((DP * TOK, DV), bf),
            pltpu.VMEM((RT, DP * TOK), bf),
            pltpu.VMEM((RV, DP * TOK), bf),
            pltpu.VMEM((TOK, DT), bf),
            pltpu.VMEM((TOK, DV), bf),
            pltpu.VMEM((TOK, DT), f32),
            pltpu.VMEM((TOK, DV), f32),
            dma((2, 4, CHUNKS)),
            dma((2, 4, 1)),
            dma((2, 4, CHUNKS)),
            dma((2, 4, CHUNKS)),
            dma((4,)),
            dma((4,)),
            dma((MB, DT // CT)),
            dma((MB,)),
            dma((2,)),
            dma((2,)),
            dma((2,)),
            dma((4,)),
        ],
        compiler_params=pltpu.CompilerParams(
            collective_id=0, has_side_effects=True, vmem_limit_bytes=60 * 1024 * 1024
        ),
        name="branches",
    )(
        t5_weight[0].T,
        vit_weight[0],
        s5,
        sv,
        s5.T,
        sv.T,
        t5_top_grad.reshape(TOK, DT),
        vit_top_grad.reshape(TOK, DV),
    )
    return (
        gv.reshape(vit_saved.shape),
        g5.reshape(t5_saved.shape),
        dv[None],
        d5[None],
    )


def solution(mesh):
    placed = (
        P("section", "dp", None),
        P("section", "dp", None),
        P("section", None, "dp", None),
        P("section", None, "dp", None),
        P(None, "dp", None),
        P(None, "dp", None),
    )
    return jax.shard_map(
        shards,
        mesh=mesh,
        in_specs=placed,
        out_specs=(
            P("section", None, "dp", None),
            P("section", None, "dp", None),
            P("section", "dp", None),
            P("section", "dp", None),
        ),
        check_vma=False,
    )
```

```python
import jax
import jax.numpy as jnp
from jax import lax
from jax.experimental import pallas as pl
from jax.experimental.pallas import tpu as pltpu
from jax.sharding import PartitionSpec as P

MESH = pl.DeviceIdType.MESH
root_half = 0.7071067811865476
inv_root_tau = 0.3989422804014327

SECTIONS = 16
DP = 16
DV = 1280
DT = 2048
RV = DV // DP
RT = DT // DP
TOK = 128
MICRO = 16
MB = TOK // MICRO
HALF = DP // 2
PARTS = 2
CHUNKS = 4
CT = 512
EARLY = 9


def slope_of(preact):
    cumulative = 0.5 * (1.0 + lax.erf(preact * root_half))
    density = jnp.exp(-0.5 * preact * preact) * inv_root_tau
    return cumulative + preact * density


def nt(a, b):
    return lax.dot_general(a, b, (((1,), (1,)), ((), ())), preferred_element_type=jnp.float32)


def nn(a, b):
    return jnp.dot(a, b, preferred_element_type=jnp.float32)


def ds(start, size, unit):
    return pl.ds(pl.multiple_of(start, unit), size)


class Gather:
    def __init__(self, slot, part, recv, pair, sent, pieces, halves):
        self.slot, self.part, self.recv, self.pair, self.sent = slot, part, recv, pair, sent
        self.pieces, self.halves = pieces, halves


def kernel(
    w5, wv, s5, sv, top5, topv,
    g5o, gvo, d5o, dvo,
    W5, WV, L5, LV, S5, SV, G5, GV, P5, PV, s5t, svt, T5, TV, R5, RV2,
    rw5, rwv, rl5, rlv, pair, sent, c5, cv, csent, asem, asent, z5, zv, zsent, lsem,
):
    s = lax.axis_index("section")
    d = lax.axis_index("dp")
    zh = lax.div(d, 8)
    x = lax.rem(lax.div(d, 2), 4)
    c = lax.rem(d, 2)
    dr = 1 - 2 * c

    def dev(half, step, core):
        return lax.rem(zh + half, 2) * 8 + lax.rem(x + step + 8, 4) * 2 + core

    nx = dev(0, dr, c)
    zp = dev(1, 0, c)
    pt = dev(0, 0, 1 - c)
    first = s == SECTIONS - 1
    lower = s > 0
    early = s < EARLY
    u = lax.rem(d, HALF)

    barrier = pltpu.get_barrier_semaphore()

    def greet(p, _):
        pl.semaphore_signal(
            barrier, inc=1, device_id=(s, lax.rem(d + p, DP)), device_id_type=MESH
        )
        return 0

    lax.fori_loop(1, DP, greet, 0)

    @pl.when(lower)
    def _():
        pl.semaphore_signal(barrier, inc=1, device_id=(s - 1, d), device_id_type=MESH)

    @pl.when(s < SECTIONS - 1)
    def _():
        pl.semaphore_signal(barrier, inc=1, device_id=(s + 1, d), device_id_type=MESH)

    W5[:, ds(d * RT, RT, RT)] = w5[...].T
    s5t[...] = s5[...].T
    svt[...] = sv[...].T
    sections = lax.div(s + SECTIONS - 1, SECTIONS) + lax.div(2 * SECTIONS - 2 - s, SECTIONS)
    pl.semaphore_wait(barrier, DP - 1 + sections)

    gw5 = Gather(
        lambda v, q: W5.at[ds(q * (DT // PARTS), DT // PARTS, 16), ds(v * RT, RT, RT)],
        lambda n: W5.at[:, pl.ds(0, n * RT)],
        rw5, pair.at[0], sent.at[0], PARTS, 2,
    )
    gwv = Gather(
        lambda v, q: WV.at[ds(v * RV, RV, 16), :],
        lambda n: WV.at[pl.ds(0, n * RV), :],
        rwv, pair.at[1], sent.at[1], 1, 2,
    )
    piece = TOK // CHUNKS
    gl5 = Gather(
        lambda v, q: L5.at[ds(lax.rem(v, HALF) * TOK + q * piece, piece, 16), :],
        lambda n: L5.at[pl.ds(0, n * TOK), :],
        rl5, pair.at[2], sent.at[2], CHUNKS, 1,
    )
    glv = Gather(
        lambda v, q: LV.at[ds(lax.rem(v, HALF) * TOK + q * piece, piece, 16), :],
        lambda n: LV.at[pl.ds(0, n * TOK), :],
        rlv, pair.at[3], sent.at[3], CHUNKS, 1,
    )

    def push(g, owner, q, recv, to):
        return pltpu.make_async_remote_copy(
            src_ref=g.slot(owner, q), dst_ref=g.slot(owner, q), send_sem=g.sent, recv_sem=recv,
            device_id=(s, to), device_id_type=MESH,
        )

    def own_ring(g, q):
        push(g, d, q, g.recv.at[0, 1, q], nx).start()

    def own_far(g, q):
        push(g, d, q, g.recv.at[1, 0, q], zp).start()

    def own_pair(g, q):
        push(g, d, q, g.pair, pt).start()

    def own(g, q):
        own_ring(g, q)
        if g.halves == 2:
            own_far(g, q)
        own_pair(g, q)

    def forward(g, h, r, q):
        owner = dev(h, -r * dr, c)
        push(g, owner, q, g.recv.at[h, r, q], nx).wait_recv()
        if r < 3:
            push(g, owner, q, g.recv.at[h, r + 1, q], nx).start()
        push(g, owner, q, g.pair, pt).start()

    def forward_when(g, h, r, q):
        @pl.when(jnp.logical_and(q >= 0, q < g.pieces))
        def _():
            forward(g, h, r, q)

    def ring_phase(g, r):
        def one(q, _):
            forward(g, 0, r, q)
            return 0

        lax.fori_loop(0, g.pieces, one, 0)

    def far_phase(g):
        def one(w, _):
            for r in range(4):
                forward_when(g, 1, r, w - r)
            return 0

        lax.fori_loop(0, g.pieces + 3, one, 0)

    def pair_done(g):
        ref = g.part(4 * g.halves)
        pltpu.make_async_copy(ref, ref, g.pair).wait()

    def sent_done(g):
        ref = g.part(8 * g.halves - 1)
        pltpu.make_async_copy(ref, ref, g.sent).wait()

    own_wv = pltpu.make_async_copy(wv, WV.at[ds(d * RV, RV, 16), :], lsem.at[0])
    own_wv.start()
    for q in range(PARTS):
        own(gw5, q)
    own_wv.wait()
    own_far(gwv, 0)

    def saved_rows(h, v):
        text = s5t.at[ds(v * RT, RT, RT), :], S5.at[pl.ds(h * RT, RT), ds(u * TOK, TOK, TOK)]
        image = svt.at[ds(v * RV, RV, 16), :], SV.at[pl.ds(h * RV, RV), ds(u * TOK, TOK, TOK)]
        return text, image

    stay = []
    for h, v in ((0, d), (1, zp)):
        for i, (src, dst) in enumerate(saved_rows(h, v)):
            stay.append(pltpu.make_async_copy(src, dst, lsem.at[2 * h + i]))
    for copy in stay:
        copy.start()
    for copy in stay:
        copy.wait()

    @pl.when(first)
    def _():
        for k in range(MB):
            rows = pl.ds(k * MICRO, MICRO)
            for n in range(DT // CT):
                cols = pl.ds(n * CT, CT)
                pltpu.make_async_copy(top5.at[rows, cols], G5.at[rows, cols], c5.at[k, n]).start()
            pltpu.make_async_copy(topv.at[rows, :], GV.at[rows, :], cv.at[k]).start()

    for r in (1, 2, 3):
        ring_phase(gw5, r)
    far_phase(gw5)
    own_ring(gwv, 0)
    own_pair(gwv, 0)
    pair_done(gw5)

    def text_slope(j, _):
        cols = ds(j * CT, CT, CT)
        P5[:, cols] = slope_of(nt(s5[...], W5[cols, :]))
        return 0

    lax.fori_loop(0, DT // CT, text_slope, 0)

    image_steps = ((1, 0), (0, 1), (1, 1), (0, 2), (1, 2), (0, 3), (1, 3))

    def image_ready():
        pair_done(gwv)

        def one(j, _):
            cols = ds(j * 256, 256, 256)
            PV[:, cols] = slope_of(nn(sv[...], WV[:, cols]))
            return 0

        lax.fori_loop(0, DV // 256, one, 0)

        def send(p, _):
            up = lax.rem(u + p, HALF)
            t = zh * HALF + up
            for h, v in ((0, t), (1, (1 - zh) * HALF + up)):
                for i, (src, dst) in enumerate(saved_rows(h, v)):
                    pltpu.make_async_remote_copy(
                        src_ref=src, dst_ref=dst, send_sem=asent.at[i], recv_sem=asem.at[i],
                        device_id=(s, t), device_id_type=MESH,
                    ).start()
            return 0

        lax.fori_loop(1, HALF, send, 0)

    @pl.when(early)
    def _():
        for h, r in image_steps:
            forward(gwv, h, r, 0)
        image_ready()

    def text_hop(k, n):
        rows, cols = ds(k * MICRO, MICRO, MICRO), pl.ds(n * CT, CT)
        return pltpu.make_async_remote_copy(
            src_ref=g5o.at[rows, cols], dst_ref=G5.at[rows, cols], send_sem=csent.at[0], recv_sem=c5.at[k, n],
            device_id=(s - 1, d), device_id_type=MESH,
        )

    def text_tick(sends):
        def tick(k, _):
            rows = ds(k * MICRO, MICRO, MICRO)
            pieces = [pl.ds(n * CT, CT) for n in range(DT // CT)]
            total = [None] * len(pieces)
            for m, inner in enumerate(pieces):
                text_hop(k, m).wait_recv()
                local = (G5[rows, inner].astype(jnp.float32) * P5[rows, inner]).astype(jnp.bfloat16)
                L5[ds(u * TOK + k * MICRO, MICRO, MICRO), inner] = local
                for n, cols in enumerate(pieces):
                    term = nn(local, W5[inner, cols])
                    total[n] = term if m == 0 else total[n] + term
                    if m == len(pieces) - 1:
                        above = G5[rows, cols].astype(jnp.float32)
                        g5o[rows, cols] = (above + total[n]).astype(jnp.bfloat16)
                        if sends:
                            text_hop(k, n).start()

            @pl.when(jnp.logical_not(early))
            def _():
                for i, (h, r) in enumerate(image_steps):

                    @pl.when(k == i)
                    def _():
                        forward(gwv, h, r, 0)

            return 0

        lax.fori_loop(0, MB, tick, 0)

    @pl.when(lower)
    def _():
        text_tick(True)

    @pl.when(jnp.logical_not(lower))
    def _():
        text_tick(False)

    @pl.when(jnp.logical_not(early))
    def _():
        image_ready()

    def image_hop(k):
        rows = ds(k * MICRO, MICRO, MICRO)
        return pltpu.make_async_remote_copy(
            src_ref=gvo.at[rows, :], dst_ref=GV.at[rows, :], send_sem=csent.at[1], recv_sem=cv.at[k],
            device_id=(s - 1, d), device_id_type=MESH,
        )

    def exchange(out, got, recv, sem, n, width):
        cols = ds(n * width, width, width)
        return pltpu.make_async_remote_copy(
            src_ref=out.at[:, cols], dst_ref=got.at[:, cols], send_sem=zsent.at[sem], recv_sem=recv.at[n],
            device_id=(s, zp), device_id_type=MESH,
        )

    def far_rows(saved, local, rows, out, got, recv, sem, width):
        def one(n, _):
            cols = ds(n * width, width, width)
            term = nn(saved[pl.ds(rows, rows), :], local[:, cols]) * (1.0 / TOK)
            out[:, cols] = term.astype(jnp.bfloat16)
            exchange(out, got, recv, sem, n, width).start()
            return 0

        lax.fori_loop(0, local.shape[1] // width, one, 0)

    def near_rows(saved, local, rows, total, width):
        def one(n, _):
            cols = ds(n * width, width, width)
            total[:, cols] = nn(saved[pl.ds(0, rows), :], local[:, cols]) * (1.0 / TOK)
            return 0

        lax.fori_loop(0, local.shape[1] // width, one, 0)

    def add_far(total, out, got, recv, sem, width):
        def one(n, _):
            cols = ds(n * width, width, width)
            exchange(out, got, recv, sem, n, width).wait_recv()
            total[:, cols] += got[:, cols].astype(jnp.float32)
            return 0

        lax.fori_loop(0, total.shape[1] // width, one, 0)

    def saved_done(ref, i):
        got = ref.at[:, pl.ds(0, (HALF - 1) * TOK)]
        pltpu.make_async_copy(got, got, asem.at[i]).wait()

    def image_tick(k, _):
        rows = ds(k * MICRO, MICRO, MICRO)
        image_hop(k).wait_recv()
        upper = GV[rows, :].astype(jnp.float32)
        local = (upper * PV[rows, :]).astype(jnp.bfloat16)
        LV[ds(u * TOK + k * MICRO, MICRO, MICRO), :] = local
        gvo[rows, :] = (upper + nt(local, WV[...])).astype(jnp.bfloat16)

        @pl.when(lower)
        def _():
            image_hop(k).start()

        return 0

    lax.fori_loop(0, MB, image_tick, 0)
    def own_all(g):
        def one(q, _):
            own(g, q)
            return 0

        lax.fori_loop(0, g.pieces, one, 0)

    own_all(gl5)
    ring_phase(gl5, 1)
    ring_phase(gl5, 2)
    own_all(glv)
    ring_phase(gl5, 3)
    pair_done(gl5)
    saved_done(S5, 0)
    far_rows(S5, L5, RT, T5, R5, z5, 0, CT)
    ring_phase(glv, 1)
    ring_phase(glv, 2)
    near_rows(S5, L5, RT, d5o, CT)
    ring_phase(glv, 3)
    pair_done(glv)
    saved_done(SV, 1)
    far_rows(SV, LV, RV, TV, RV2, zv, 1, 256)
    near_rows(SV, LV, RV, dvo, 256)
    add_far(d5o, T5, R5, z5, 0, CT)
    add_far(dvo, TV, RV2, zv, 1, 256)
    for g in (gw5, gwv, gl5, glv):
        sent_done(g)
    for i, (ref, size) in enumerate(((s5t, RT), (svt, RV))):
        gone = ref.at[pl.ds(0, 2 * (HALF - 1) * size), :]
        pltpu.make_async_copy(gone, gone, asent.at[i]).wait()
    pltpu.make_async_copy(T5, T5, zsent.at[0]).wait()
    pltpu.make_async_copy(TV, TV, zsent.at[1]).wait()

    @pl.when(lower)
    def _():
        pltpu.make_async_copy(g5o, g5o, csent.at[0]).wait()
        pltpu.make_async_copy(gvo, gvo, csent.at[1]).wait()


def shards(vit_weight, t5_weight, vit_saved, t5_saved, vit_top_grad, t5_top_grad):
    bf, f32 = jnp.bfloat16, jnp.float32
    dma, vmem = pltpu.SemaphoreType.DMA, pl.BlockSpec(memory_space=pltpu.VMEM)
    g5, gv, d5, dv = pl.pallas_call(
        kernel,
        out_shape=(
            jax.ShapeDtypeStruct((TOK, DT), bf),
            jax.ShapeDtypeStruct((TOK, DV), bf),
            jax.ShapeDtypeStruct((RT, DT), f32),
            jax.ShapeDtypeStruct((RV, DV), f32),
        ),
        in_specs=[vmem] * 6,
        out_specs=[vmem] * 4,
        scratch_shapes=[
            pltpu.VMEM((DT, DT), bf),
            pltpu.VMEM((DV, DV), bf),
            pltpu.VMEM((HALF * TOK, DT), bf),
            pltpu.VMEM((HALF * TOK, DV), bf),
            pltpu.VMEM((2 * RT, HALF * TOK), bf),
            pltpu.VMEM((2 * RV, HALF * TOK), bf),
            pltpu.VMEM((TOK, DT), bf),
            pltpu.VMEM((TOK, DV), bf),
            pltpu.VMEM((TOK, DT), f32),
            pltpu.VMEM((TOK, DV), f32),
            pltpu.VMEM((DT, TOK), bf),
            pltpu.VMEM((DV, TOK), bf),
            pltpu.VMEM((RT, DT), bf),
            pltpu.VMEM((RV, DV), bf),
            pltpu.VMEM((RT, DT), bf),
            pltpu.VMEM((RV, DV), bf),
            dma((2, 4, PARTS)),
            dma((2, 4, 1)),
            dma((1, 4, CHUNKS)),
            dma((1, 4, CHUNKS)),
            dma((4,)),
            dma((4,)),
            dma((MB, DT // CT)),
            dma((MB,)),
            dma((2,)),
            dma((2,)),
            dma((2,)),
            dma((DT // CT,)),
            dma((DV // 256,)),
            dma((2,)),
            dma((4,)),
        ],
        compiler_params=pltpu.CompilerParams(
            collective_id=0, has_side_effects=True, vmem_limit_bytes=60 * 1024 * 1024
        ),
        name="branches",
    )(
        t5_weight[0],
        vit_weight[0],
        t5_saved.reshape(TOK, DT),
        vit_saved.reshape(TOK, DV),
        t5_top_grad.reshape(TOK, DT),
        vit_top_grad.reshape(TOK, DV),
    )
    return (
        gv.reshape(vit_saved.shape),
        g5.reshape(t5_saved.shape),
        dv[None],
        d5[None],
    )


def solution(mesh):
    placed = (
        P("section", "dp", None),
        P("section", "dp", None),
        P("section", None, "dp", None),
        P("section", None, "dp", None),
        P(None, "dp", None),
        P(None, "dp", None),
    )
    return jax.shard_map(
        shards,
        mesh=mesh,
        in_specs=placed,
        out_specs=(
            P("section", None, "dp", None),
            P("section", None, "dp", None),
            P("section", "dp", None),
            P("section", "dp", None),
        ),
        check_vma=False,
    )
```

```python
import jax
import jax.numpy as jnp
from jax import lax
from jax.experimental import pallas as pl
from jax.experimental.pallas import tpu as pltpu
from jax.sharding import PartitionSpec as P

MESH = pl.DeviceIdType.MESH
root_half = 0.7071067811865476
inv_root_tau = 0.3989422804014327

SECTIONS = 16
DP = 16
DV = 1280
DT = 2048
RV = DV // DP
RT = DT // DP
TOK = 128
MICRO = 16
MB = TOK // MICRO
HALF = DP // 2
PARTS = 2
CHUNKS = 8
CHUNKS_V = 2
CT = 512
EARLY = 9


def slope_of(preact):
    cumulative = 0.5 * (1.0 + lax.erf(preact * root_half))
    density = jnp.exp(-0.5 * preact * preact) * inv_root_tau
    return cumulative + preact * density


def nt(a, b):
    return lax.dot_general(a, b, (((1,), (1,)), ((), ())), preferred_element_type=jnp.float32)


def nn(a, b):
    return jnp.dot(a, b, preferred_element_type=jnp.float32)


def ds(start, size, unit):
    return pl.ds(pl.multiple_of(start, unit), size)


class Gather:
    def __init__(self, slot, part, recv, pair, sent, pieces, halves):
        self.slot, self.part, self.recv, self.pair, self.sent = slot, part, recv, pair, sent
        self.pieces, self.halves = pieces, halves


def kernel(
    w5, wv, s5, sv, top5, topv,
    g5o, gvo, d5o, dvo,
    W5, WV, L5, LV, S5, SV, G5, GV, P5, PV, s5t, svt, T5, TV, R5, RV2, WT,
    rw5, rwv, rl5, rlv, pair, sent, c5, cv, csent, asem, asent, z5, zv, zsent, lsem,
):
    s = lax.axis_index("section")
    d = lax.axis_index("dp")
    zh = lax.div(d, 8)
    x = lax.rem(lax.div(d, 2), 4)
    c = lax.rem(d, 2)
    dr = 1 - 2 * c

    def dev(half, step, core):
        return lax.rem(zh + half, 2) * 8 + lax.rem(x + step + 8, 4) * 2 + core

    nx = dev(0, dr, c)
    zp = dev(1, 0, c)
    pt = dev(0, 0, 1 - c)
    first = s == SECTIONS - 1
    lower = s > 0
    early = s < EARLY
    u = lax.rem(d, HALF)

    barrier = pltpu.get_barrier_semaphore()

    def greet(p, _):
        pl.semaphore_signal(
            barrier, inc=1, device_id=(s, lax.rem(d + p, DP)), device_id_type=MESH
        )
        return 0

    lax.fori_loop(1, DP, greet, 0)

    @pl.when(lower)
    def _():
        pl.semaphore_signal(barrier, inc=1, device_id=(s - 1, d), device_id_type=MESH)

    @pl.when(s < SECTIONS - 1)
    def _():
        pl.semaphore_signal(barrier, inc=1, device_id=(s + 1, d), device_id_type=MESH)

    W5[:, ds(d * RT, RT, RT)] = w5[...].T
    sections = lax.div(s + SECTIONS - 1, SECTIONS) + lax.div(2 * SECTIONS - 2 - s, SECTIONS)
    pl.semaphore_wait(barrier, DP - 1 + sections)

    gw5 = Gather(
        lambda v, q: W5.at[ds(q * (DT // PARTS), DT // PARTS, 16), ds(v * RT, RT, RT)],
        lambda n: W5.at[:, pl.ds(0, n * RT)],
        rw5, pair.at[0], sent.at[0], PARTS, 2,
    )
    gwv = Gather(
        lambda v, q: WV.at[ds(v * RV, RV, 16), :],
        lambda n: WV.at[pl.ds(0, n * RV), :],
        rwv, pair.at[1], sent.at[1], 1, 2,
    )
    piece = TOK // CHUNKS
    gl5 = Gather(
        lambda v, q: L5.at[ds(lax.rem(v, HALF) * TOK + q * piece, piece, 16), :],
        lambda n: L5.at[pl.ds(0, n * TOK), :],
        rl5, pair.at[2], sent.at[2], CHUNKS, 1,
    )
    glv = Gather(
        lambda v, q: LV.at[ds(lax.rem(v, HALF) * TOK + q * (TOK // CHUNKS_V), TOK // CHUNKS_V, 16), :],
        lambda n: LV.at[pl.ds(0, n * TOK), :],
        rlv, pair.at[3], sent.at[3], CHUNKS_V, 1,
    )

    def push(g, owner, q, recv, to):
        return pltpu.make_async_remote_copy(
            src_ref=g.slot(owner, q), dst_ref=g.slot(owner, q), send_sem=g.sent, recv_sem=recv,
            device_id=(s, to), device_id_type=MESH,
        )

    def own_ring(g, q):
        push(g, d, q, g.recv.at[0, 1, q], nx).start()

    def own_far(g, q):
        push(g, d, q, g.recv.at[1, 0, q], zp).start()

    def own_pair(g, q):
        push(g, d, q, g.pair, pt).start()

    def own(g, q):
        own_ring(g, q)
        if g.halves == 2:
            own_far(g, q)
        own_pair(g, q)

    def forward(g, h, r, q):
        owner = dev(h, -r * dr, c)
        push(g, owner, q, g.recv.at[h, r, q], nx).wait_recv()
        if r < 3:
            push(g, owner, q, g.recv.at[h, r + 1, q], nx).start()
        push(g, owner, q, g.pair, pt).start()

    def forward_when(g, h, r, q):
        @pl.when(jnp.logical_and(q >= 0, q < g.pieces))
        def _():
            forward(g, h, r, q)

    def ring_phase(g, r):
        def one(q, _):
            forward(g, 0, r, q)
            return 0

        lax.fori_loop(0, g.pieces, one, 0)

    def far_phase(g):
        def one(w, _):
            for r in range(4):
                forward_when(g, 1, r, w - r)
            return 0

        lax.fori_loop(0, g.pieces + 3, one, 0)

    def pair_done(g):
        ref = g.part(4 * g.halves)
        pltpu.make_async_copy(ref, ref, g.pair).wait()

    def sent_done(g):
        ref = g.part(8 * g.halves - 1)
        pltpu.make_async_copy(ref, ref, g.sent).wait()

    own_wv = pltpu.make_async_copy(wv, WV.at[ds(d * RV, RV, 16), :], lsem.at[0])
    own_wv.start()
    for q in range(PARTS):
        own(gw5, q)
    own_wv.wait()
    own_far(gwv, 0)
    s5t[...] = s5[...].T
    svt[...] = sv[...].T

    def saved_rows(h, v):
        text = s5t.at[ds(v * RT, RT, RT), :], S5.at[pl.ds(h * RT, RT), ds(u * TOK, TOK, TOK)]
        image = svt.at[ds(v * RV, RV, 16), :], SV.at[pl.ds(h * RV, RV), ds(u * TOK, TOK, TOK)]
        return text, image

    stay = []
    for h, v in ((0, d), (1, zp)):
        for i, (src, dst) in enumerate(saved_rows(h, v)):
            stay.append(pltpu.make_async_copy(src, dst, lsem.at[2 * h + i]))
    for copy in stay:
        copy.start()
    for copy in stay:
        copy.wait()

    @pl.when(first)
    def _():
        for k in range(MB):
            rows = pl.ds(k * MICRO, MICRO)
            for n in range(DT // CT):
                cols = pl.ds(n * CT, CT)
                pltpu.make_async_copy(top5.at[rows, cols], G5.at[rows, cols], c5.at[k, n]).start()
            pltpu.make_async_copy(topv.at[rows, :], GV.at[rows, :], cv.at[k]).start()

    for r in (1, 2, 3):
        ring_phase(gw5, r)
    far_phase(gw5)
    own_ring(gwv, 0)
    own_pair(gwv, 0)
    pair_done(gw5)

    def text_slope(j, _):
        cols = ds(j * CT, CT, CT)
        P5[:, cols] = slope_of(nt(s5[...], W5[cols, :]))
        return 0

    lax.fori_loop(0, DT // CT, text_slope, 0)

    image_steps = ((1, 0), (0, 1), (1, 1), (0, 2), (1, 2), (0, 3), (1, 3))

    def image_ready():
        pair_done(gwv)
        WT[...] = WV[...].T

        def one(j, _):
            cols = ds(j * 256, 256, 256)
            PV[:, cols] = slope_of(nn(sv[...], WV[:, cols]))
            return 0

        lax.fori_loop(0, DV // 256, one, 0)

        def send(p, _):
            up = lax.rem(u + p, HALF)
            t = zh * HALF + up
            for h, v in ((0, t), (1, (1 - zh) * HALF + up)):
                for i, (src, dst) in enumerate(saved_rows(h, v)):
                    pltpu.make_async_remote_copy(
                        src_ref=src, dst_ref=dst, send_sem=asent.at[i], recv_sem=asem.at[i],
                        device_id=(s, t), device_id_type=MESH,
                    ).start()
            return 0

        lax.fori_loop(1, HALF, send, 0)

    @pl.when(early)
    def _():
        for h, r in image_steps:
            forward(gwv, h, r, 0)
        image_ready()

    def text_hop(k, n):
        rows, cols = ds(k * MICRO, MICRO, MICRO), pl.ds(n * CT, CT)
        return pltpu.make_async_remote_copy(
            src_ref=g5o.at[rows, cols], dst_ref=G5.at[rows, cols], send_sem=csent.at[0], recv_sem=c5.at[k, n],
            device_id=(s - 1, d), device_id_type=MESH,
        )

    def text_tick(sends):
        def tick(k, _):
            rows = ds(k * MICRO, MICRO, MICRO)
            pieces = [pl.ds(n * CT, CT) for n in range(DT // CT)]
            total = [None] * len(pieces)
            for m, inner in enumerate(pieces):
                text_hop(k, m).wait_recv()
                local = (G5[rows, inner].astype(jnp.float32) * P5[rows, inner]).astype(jnp.bfloat16)
                L5[ds(u * TOK + k * MICRO, MICRO, MICRO), inner] = local
                for n, cols in enumerate(pieces):
                    term = nn(local, W5[inner, cols])
                    total[n] = term if m == 0 else total[n] + term
                    if m == len(pieces) - 1:
                        above = G5[rows, cols].astype(jnp.float32)
                        g5o[rows, cols] = (above + total[n]).astype(jnp.bfloat16)
                        if sends:
                            text_hop(k, n).start()

            own(gl5, k)

            @pl.when(jnp.logical_not(early))
            def _():
                for i, (h, r) in enumerate(image_steps):

                    @pl.when(k == i)
                    def _():
                        forward(gwv, h, r, 0)

            return 0

        lax.fori_loop(0, MB, tick, 0)

    @pl.when(lower)
    def _():
        text_tick(True)

    @pl.when(jnp.logical_not(lower))
    def _():
        text_tick(False)

    @pl.when(jnp.logical_not(early))
    def _():
        image_ready()

    def image_hop(k):
        rows = ds(k * MICRO, MICRO, MICRO)
        return pltpu.make_async_remote_copy(
            src_ref=gvo.at[rows, :], dst_ref=GV.at[rows, :], send_sem=csent.at[1], recv_sem=cv.at[k],
            device_id=(s - 1, d), device_id_type=MESH,
        )

    def exchange(out, got, recv, sem, n, width):
        cols = ds(n * width, width, width)
        return pltpu.make_async_remote_copy(
            src_ref=out.at[:, cols], dst_ref=got.at[:, cols], send_sem=zsent.at[sem], recv_sem=recv.at[n],
            device_id=(s, zp), device_id_type=MESH,
        )

    def far_rows(saved, local, rows, out, got, recv, sem, width):
        def one(n, _):
            cols = ds(n * width, width, width)
            term = nn(saved[pl.ds(rows, rows), :], local[:, cols]) * (1.0 / TOK)
            out[:, cols] = term.astype(jnp.bfloat16)
            exchange(out, got, recv, sem, n, width).start()
            return 0

        lax.fori_loop(0, local.shape[1] // width, one, 0)

    def near_rows(saved, local, rows, total, width):
        def one(n, _):
            cols = ds(n * width, width, width)
            total[:, cols] = nn(saved[pl.ds(0, rows), :], local[:, cols]) * (1.0 / TOK)
            return 0

        lax.fori_loop(0, local.shape[1] // width, one, 0)

    def add_far(total, out, got, recv, sem, width):
        def one(n, _):
            cols = ds(n * width, width, width)
            exchange(out, got, recv, sem, n, width).wait_recv()
            total[:, cols] += got[:, cols].astype(jnp.float32)
            return 0

        lax.fori_loop(0, total.shape[1] // width, one, 0)

    def saved_done(ref, i):
        got = ref.at[:, pl.ds(0, (HALF - 1) * TOK)]
        pltpu.make_async_copy(got, got, asem.at[i]).wait()

    def image_tick(k, _):
        rows = ds(k * MICRO, MICRO, MICRO)
        image_hop(k).wait_recv()
        upper = GV[rows, :].astype(jnp.float32)
        local = (upper * PV[rows, :]).astype(jnp.bfloat16)
        LV[ds(u * TOK + k * MICRO, MICRO, MICRO), :] = local
        gvo[rows, :] = (upper + nn(local, WT[...])).astype(jnp.bfloat16)

        @pl.when(lower)
        def _():
            image_hop(k).start()

        forward(gl5, 0, 1, k)

        return 0

    lax.fori_loop(0, MB, image_tick, 0)
    def own_all(g):
        def one(q, _):
            own(g, q)
            return 0

        lax.fori_loop(0, g.pieces, one, 0)

    ring_phase(gl5, 2)
    own_all(glv)
    ring_phase(gl5, 3)
    pair_done(gl5)
    saved_done(S5, 0)
    far_rows(S5, L5, RT, T5, R5, z5, 0, CT)
    ring_phase(glv, 1)
    ring_phase(glv, 2)
    near_rows(S5, L5, RT, d5o, CT)
    ring_phase(glv, 3)
    pair_done(glv)
    saved_done(SV, 1)
    far_rows(SV, LV, RV, TV, RV2, zv, 1, 256)
    near_rows(SV, LV, RV, dvo, 256)
    add_far(d5o, T5, R5, z5, 0, CT)
    add_far(dvo, TV, RV2, zv, 1, 256)
    for g in (gw5, gwv, gl5, glv):
        sent_done(g)
    for i, (ref, size) in enumerate(((s5t, RT), (svt, RV))):
        gone = ref.at[pl.ds(0, 2 * (HALF - 1) * size), :]
        pltpu.make_async_copy(gone, gone, asent.at[i]).wait()
    pltpu.make_async_copy(T5, T5, zsent.at[0]).wait()
    pltpu.make_async_copy(TV, TV, zsent.at[1]).wait()

    @pl.when(lower)
    def _():
        pltpu.make_async_copy(g5o, g5o, csent.at[0]).wait()
        pltpu.make_async_copy(gvo, gvo, csent.at[1]).wait()


def shards(vit_weight, t5_weight, vit_saved, t5_saved, vit_top_grad, t5_top_grad):
    bf, f32 = jnp.bfloat16, jnp.float32
    dma, vmem = pltpu.SemaphoreType.DMA, pl.BlockSpec(memory_space=pltpu.VMEM)
    g5, gv, d5, dv = pl.pallas_call(
        kernel,
        out_shape=(
            jax.ShapeDtypeStruct((TOK, DT), bf),
            jax.ShapeDtypeStruct((TOK, DV), bf),
            jax.ShapeDtypeStruct((RT, DT), f32),
            jax.ShapeDtypeStruct((RV, DV), f32),
        ),
        in_specs=[vmem] * 6,
        out_specs=[vmem] * 4,
        scratch_shapes=[
            pltpu.VMEM((DT, DT), bf),
            pltpu.VMEM((DV, DV), bf),
            pltpu.VMEM((HALF * TOK, DT), bf),
            pltpu.VMEM((HALF * TOK, DV), bf),
            pltpu.VMEM((2 * RT, HALF * TOK), bf),
            pltpu.VMEM((2 * RV, HALF * TOK), bf),
            pltpu.VMEM((TOK, DT), bf),
            pltpu.VMEM((TOK, DV), bf),
            pltpu.VMEM((TOK, DT), f32),
            pltpu.VMEM((TOK, DV), f32),
            pltpu.VMEM((DT, TOK), bf),
            pltpu.VMEM((DV, TOK), bf),
            pltpu.VMEM((RT, DT), bf),
            pltpu.VMEM((RV, DV), bf),
            pltpu.VMEM((RT, DT), bf),
            pltpu.VMEM((RV, DV), bf),
            pltpu.VMEM((DV, DV), bf),
            dma((2, 4, PARTS)),
            dma((2, 4, 1)),
            dma((1, 4, CHUNKS)),
            dma((1, 4, CHUNKS_V)),
            dma((4,)),
            dma((4,)),
            dma((MB, DT // CT)),
            dma((MB,)),
            dma((2,)),
            dma((2,)),
            dma((2,)),
            dma((DT // CT,)),
            dma((DV // 256,)),
            dma((2,)),
            dma((4,)),
        ],
        compiler_params=pltpu.CompilerParams(
            collective_id=0, has_side_effects=True, vmem_limit_bytes=60 * 1024 * 1024
        ),
        name="branches",
    )(
        t5_weight[0],
        vit_weight[0],
        t5_saved.reshape(TOK, DT),
        vit_saved.reshape(TOK, DV),
        t5_top_grad.reshape(TOK, DT),
        vit_top_grad.reshape(TOK, DV),
    )
    return (
        gv.reshape(vit_saved.shape),
        g5.reshape(t5_saved.shape),
        dv[None],
        d5[None],
    )


def solution(mesh):
    placed = (
        P("section", "dp", None),
        P("section", "dp", None),
        P("section", None, "dp", None),
        P("section", None, "dp", None),
        P(None, "dp", None),
        P(None, "dp", None),
    )
    return jax.shard_map(
        shards,
        mesh=mesh,
        in_specs=placed,
        out_specs=(
            P("section", None, "dp", None),
            P("section", None, "dp", None),
            P("section", "dp", None),
            P("section", "dp", None),
        ),
        check_vma=False,
    )
```

```python
import jax
import jax.numpy as jnp
from jax import lax
from jax.experimental import pallas as pl
from jax.experimental.pallas import tpu as pltpu
from jax.sharding import PartitionSpec as P

MESH = pl.DeviceIdType.MESH
root_half = 0.7071067811865476
inv_root_tau = 0.3989422804014327

SECTIONS = 16
DP = 16
DV = 1280
DT = 2048
RV = DV // DP
RT = DT // DP
TOK = 128
MICRO = 16
MB = TOK // MICRO
HALF = DP // 2
PARTS = 2
CHUNKS = 8
CHUNKS_V = 2
CT = 512
RELAYED = 2
ROW = 4
RELAY = SECTIONS - ROW
KEPT = (2, 3)
EAGER = 2
LAG = 3
EARLY = 9


def slope_of(preact):
    cumulative = 0.5 * (1.0 + lax.erf(preact * root_half))
    density = jnp.exp(-0.5 * preact * preact) * inv_root_tau
    return cumulative + preact * density


def nt(a, b):
    return lax.dot_general(a, b, (((1,), (1,)), ((), ())), preferred_element_type=jnp.float32)


def nn(a, b):
    return jnp.dot(a, b, preferred_element_type=jnp.float32)


def ds(start, size, unit):
    return pl.ds(pl.multiple_of(start, unit), size)


class Gather:
    def __init__(self, slot, part, recv, pair, sent, pieces, halves):
        self.slot, self.part, self.recv, self.pair, self.sent = slot, part, recv, pair, sent
        self.pieces, self.halves = pieces, halves


def kernel(
    w5, wv, s5, sv, top5, topv,
    g5o, gvo, d5o, dvo,
    W5, WV, L5, LV, S5, SV, G5, GV, P5, PV, s5t, svt, T5, TV, R5, RV2, WT, QT, QV, FT, FV,
    rw5, rwv, rl5, rlv, pair, sent, c5, cv, csent, asem, asent, z5, zv, zsent, lsem, rq, rsent,
):
    s = lax.axis_index("section")
    d = lax.axis_index("dp")
    zh = lax.div(d, 8)
    x = lax.rem(lax.div(d, 2), 4)
    c = lax.rem(d, 2)
    dr = 1 - 2 * c

    def dev(half, step, core):
        return lax.rem(zh + half, 2) * 8 + lax.rem(x + step + 8, 4) * 2 + core

    nx = dev(0, dr, c)
    zp = dev(1, 0, c)
    pt = dev(0, 0, 1 - c)
    first = s == SECTIONS - 1
    lower = s > 0
    early = s < EARLY
    eager = s < EAGER
    u = lax.rem(d, HALF)

    barrier = pltpu.get_barrier_semaphore()

    def greet(p, _):
        pl.semaphore_signal(
            barrier, inc=1, device_id=(s, lax.rem(d + p, DP)), device_id_type=MESH
        )
        return 0

    lax.fori_loop(1, DP, greet, 0)

    @pl.when(lower)
    def _():
        pl.semaphore_signal(barrier, inc=1, device_id=(s - 1, d), device_id_type=MESH)

    @pl.when(s < SECTIONS - 1)
    def _():
        pl.semaphore_signal(barrier, inc=1, device_id=(s + 1, d), device_id_type=MESH)

    W5[:, ds(d * RT, RT, RT)] = w5[...].T
    @pl.when(s < RELAYED)
    def _():
        pl.semaphore_signal(barrier, inc=1, device_id=(s + RELAY, d), device_id_type=MESH)

    @pl.when(jnp.logical_and(s >= RELAY, s < RELAY + RELAYED))
    def _():
        pl.semaphore_signal(barrier, inc=1, device_id=(s - RELAY, d), device_id_type=MESH)

    helps = jnp.logical_or(s < RELAYED, jnp.logical_and(s >= RELAY, s < RELAY + RELAYED))
    sections = helps.astype(jnp.int32)
    sections += lax.div(s + SECTIONS - 1, SECTIONS) + lax.div(2 * SECTIONS - 2 - s, SECTIONS)
    pl.semaphore_wait(barrier, DP - 1 + sections)

    gw5 = Gather(
        lambda v, q: W5.at[ds(q * (DT // PARTS), DT // PARTS, 16), ds(v * RT, RT, RT)],
        lambda n: W5.at[:, pl.ds(0, n * RT)],
        rw5, pair.at[0], sent.at[0], PARTS, 2,
    )
    gwv = Gather(
        lambda v, q: WV.at[ds(v * RV, RV, 16), :],
        lambda n: WV.at[pl.ds(0, n * RV), :],
        rwv, pair.at[1], sent.at[1], 1, 2,
    )
    piece = TOK // CHUNKS
    gl5 = Gather(
        lambda v, q: L5.at[ds(lax.rem(v, HALF) * TOK + q * piece, piece, 16), :],
        lambda n: L5.at[pl.ds(0, n * TOK), :],
        rl5, pair.at[2], sent.at[2], CHUNKS, 1,
    )
    glv = Gather(
        lambda v, q: LV.at[ds(lax.rem(v, HALF) * TOK + q * (TOK // CHUNKS_V), TOK // CHUNKS_V, 16), :],
        lambda n: LV.at[pl.ds(0, n * TOK), :],
        rlv, pair.at[3], sent.at[3], CHUNKS_V, 1,
    )

    def push(g, owner, q, recv, to):
        return pltpu.make_async_remote_copy(
            src_ref=g.slot(owner, q), dst_ref=g.slot(owner, q), send_sem=g.sent, recv_sem=recv,
            device_id=(s, to), device_id_type=MESH,
        )

    def own_ring(g, q):
        push(g, d, q, g.recv.at[0, 1, q], nx).start()

    def own_far(g, q):
        push(g, d, q, g.recv.at[1, 0, q], zp).start()

    def own_pair(g, q):
        push(g, d, q, g.pair, pt).start()

    def own(g, q):
        own_ring(g, q)
        if g.halves == 2:
            own_far(g, q)
        own_pair(g, q)

    def forward(g, h, r, q):
        owner = dev(h, -r * dr, c)
        push(g, owner, q, g.recv.at[h, r, q], nx).wait_recv()
        if r < 3:
            push(g, owner, q, g.recv.at[h, r + 1, q], nx).start()
        push(g, owner, q, g.pair, pt).start()

    def forward_when(g, h, r, q):
        @pl.when(jnp.logical_and(q >= 0, q < g.pieces))
        def _():
            forward(g, h, r, q)

    def ring_phase(g, r):
        def one(q, _):
            forward(g, 0, r, q)
            return 0

        lax.fori_loop(0, g.pieces, one, 0)

    def far_phase(g):
        def one(w, _):
            for r in range(4):
                forward_when(g, 1, r, w - r)
            return 0

        lax.fori_loop(0, g.pieces + 3, one, 0)

    def pair_done(g):
        ref = g.part(4 * g.halves)
        pltpu.make_async_copy(ref, ref, g.pair).wait()

    def sent_done(g):
        ref = g.part(8 * g.halves - 1)
        pltpu.make_async_copy(ref, ref, g.sent).wait()

    own_wv = pltpu.make_async_copy(wv, WV.at[ds(d * RV, RV, 16), :], lsem.at[0])
    own_wv.start()
    for q in range(PARTS):
        own(gw5, q)
    own_wv.wait()
    own_far(gwv, 0)
    s5t[...] = s5[...].T
    svt[...] = sv[...].T

    def saved_rows(h, v):
        text = s5t.at[ds(v * RT, RT, RT), :], S5.at[pl.ds(h * RT, RT), ds(u * TOK, TOK, TOK)]
        image = svt.at[ds(v * RV, RV, 16), :], SV.at[pl.ds(h * RV, RV), ds(u * TOK, TOK, TOK)]
        return text, image

    stay = []
    for h, v in ((0, d), (1, zp)):
        for i, (src, dst) in enumerate(saved_rows(h, v)):
            stay.append(pltpu.make_async_copy(src, dst, lsem.at[2 * h + i]))
    for copy in stay:
        copy.start()
    for copy in stay:
        copy.wait()

    @pl.when(first)
    def _():
        for k in range(MB):
            rows = pl.ds(k * MICRO, MICRO)
            for n in range(DT // CT):
                cols = pl.ds(n * CT, CT)
                pltpu.make_async_copy(top5.at[rows, cols], G5.at[rows, cols], c5.at[k, n]).start()
            pltpu.make_async_copy(topv.at[rows, :], GV.at[rows, :], cv.at[k]).start()

    for r in (1, 2, 3):
        ring_phase(gw5, r)
    far_phase(gw5)
    own_ring(gwv, 0)
    own_pair(gwv, 0)
    pair_done(gw5)

    def text_slope(j, _):
        cols = ds(j * CT, CT, CT)
        P5[:, cols] = slope_of(nt(s5[...], W5[cols, :]))
        return 0

    lax.fori_loop(0, DT // CT, text_slope, 0)

    image_steps = ((1, 0), (0, 1), (1, 1), (0, 2), (1, 2), (0, 3), (1, 3))

    def image_ready():
        pair_done(gwv)
        WT[...] = WV[...].T

        def one(j, _):
            cols = ds(j * 256, 256, 256)
            PV[:, cols] = slope_of(nn(sv[...], WV[:, cols]))
            return 0

        lax.fori_loop(0, DV // 256, one, 0)

        def send(p, _):
            up = lax.rem(u + p, HALF)
            t = zh * HALF + up
            for h, v in ((0, t), (1, (1 - zh) * HALF + up)):
                for i, (src, dst) in enumerate(saved_rows(h, v)):
                    pltpu.make_async_remote_copy(
                        src_ref=src, dst_ref=dst, send_sem=asent.at[i], recv_sem=asem.at[i],
                        device_id=(s, t), device_id_type=MESH,
                    ).start()
            return 0

        lax.fori_loop(1, HALF, send, 0)

    @pl.when(early)
    def _():
        for h, r in image_steps:
            forward(gwv, h, r, 0)
        image_ready()

    def text_hop(k, n):
        rows, cols = ds(k * MICRO, MICRO, MICRO), pl.ds(n * CT, CT)
        return pltpu.make_async_remote_copy(
            src_ref=g5o.at[rows, cols], dst_ref=G5.at[rows, cols], send_sem=csent.at[0], recv_sem=c5.at[k, n],
            device_id=(s - 1, d), device_id_type=MESH,
        )

    def text_tick(sends):
        def tick(k, _):
            rows = ds(k * MICRO, MICRO, MICRO)
            pieces = [pl.ds(n * CT, CT) for n in range(DT // CT)]
            total = [None] * len(pieces)
            for m, inner in enumerate(pieces):
                text_hop(k, m).wait_recv()
                local = (G5[rows, inner].astype(jnp.float32) * P5[rows, inner]).astype(jnp.bfloat16)
                L5[ds(u * TOK + k * MICRO, MICRO, MICRO), inner] = local
                for n, cols in enumerate(pieces):
                    term = nn(local, W5[inner, cols])
                    total[n] = term if m == 0 else total[n] + term
                    if m == len(pieces) - 1:
                        above = G5[rows, cols].astype(jnp.float32)
                        g5o[rows, cols] = (above + total[n]).astype(jnp.bfloat16)
                        if sends:
                            text_hop(k, n).start()

            own(gl5, k)

            @pl.when(eager)
            def _():
                forward_when(gl5, 0, 1, k - LAG)

            @pl.when(jnp.logical_not(early))
            def _():
                for i, (h, r) in enumerate(image_steps):

                    @pl.when(k == i)
                    def _():
                        forward(gwv, h, r, 0)

            return 0

        lax.fori_loop(0, MB, tick, 0)

    @pl.when(lower)
    def _():
        text_tick(True)

    @pl.when(jnp.logical_not(lower))
    def _():
        text_tick(False)

    @pl.when(jnp.logical_not(early))
    def _():
        image_ready()

    def image_hop(k):
        rows = ds(k * MICRO, MICRO, MICRO)
        return pltpu.make_async_remote_copy(
            src_ref=gvo.at[rows, :], dst_ref=GV.at[rows, :], send_sem=csent.at[1], recv_sem=cv.at[k],
            device_id=(s - 1, d), device_id_type=MESH,
        )

    def exchange(out, got, recv, sem, n, width):
        cols = ds(n * width, width, width)
        return pltpu.make_async_remote_copy(
            src_ref=out.at[:, cols], dst_ref=got.at[:, cols], send_sem=zsent.at[sem], recv_sem=recv.at[n],
            device_id=(s, zp), device_id_type=MESH,
        )

    def away(stage, kind, i):
        width = (CT, 256)[kind]
        here, there = pl.ds(i * width, width), pl.ds((i + KEPT[kind]) * width, width)
        out, first_stop, second_stop, got = ((T5, QT, FT, R5), (TV, QV, FV, RV2))[kind]
        src = (out.at[:, there], first_stop.at[:, here], second_stop.at[:, here])[stage]
        dst = (first_stop.at[:, here], second_stop.at[:, here], got.at[:, there])[stage]
        recv = rq.at[stage, kind, i] if stage < 2 else (z5, zv)[kind].at[i + KEPT[kind]]
        to = ((s + RELAY, d), (s, zp), (s - RELAY, d))[stage]
        return pltpu.make_async_remote_copy(
            src_ref=src, dst_ref=dst, send_sem=zsent.at[kind] if stage == 0 else rsent.at[stage - 1, kind, i],
            recv_sem=recv, device_id=to, device_id_type=MESH,
        )

    def far_rows(saved, local, rows, out, got, recv, sem, width):
        def one(n, _):
            cols = ds(n * width, width, width)
            term = nn(saved[pl.ds(rows, rows), :], local[:, cols]) * (1.0 / TOK)
            out[:, cols] = term.astype(jnp.bfloat16)
            far = jnp.logical_and(s < RELAYED, n >= KEPT[sem])

            @pl.when(jnp.logical_not(far))
            def _():
                exchange(out, got, recv, sem, n, width).start()

            for i in range(2):

                @pl.when(jnp.logical_and(far, n == i + KEPT[sem]))
                def _():
                    away(0, sem, i).start()

            return 0

        lax.fori_loop(0, local.shape[1] // width, one, 0)

    def near_rows(saved, local, rows, total, width):
        def one(n, _):
            cols = ds(n * width, width, width)
            total[:, cols] = nn(saved[pl.ds(0, rows), :], local[:, cols]) * (1.0 / TOK)
            return 0

        lax.fori_loop(0, local.shape[1] // width, one, 0)

    def add_far(total, out, got, recv, sem, width):
        def one(n, _):
            cols = ds(n * width, width, width)
            exchange(out, got, recv, sem, n, width).wait_recv()
            total[:, cols] += got[:, cols].astype(jnp.float32)
            return 0

        lax.fori_loop(0, total.shape[1] // width, one, 0)

    def saved_done(ref, i):
        got = ref.at[:, pl.ds(0, (HALF - 1) * TOK)]
        pltpu.make_async_copy(got, got, asem.at[i]).wait()

    def image_tick(k, _):
        rows = ds(k * MICRO, MICRO, MICRO)
        image_hop(k).wait_recv()
        upper = GV[rows, :].astype(jnp.float32)
        local = (upper * PV[rows, :]).astype(jnp.bfloat16)
        LV[ds(u * TOK + k * MICRO, MICRO, MICRO), :] = local
        gvo[rows, :] = (upper + nn(local, WT[...])).astype(jnp.bfloat16)

        @pl.when(lower)
        def _():
            image_hop(k).start()


        @pl.when(jnp.logical_or(jnp.logical_not(eager), k < LAG))
        def _():
            forward(gl5, 0, 1, k + jnp.where(eager, MB - LAG, 0))

        @pl.when(eager)
        def _():
            forward(gl5, 0, 2, k)

            @pl.when(lax.rem(k, MB // CHUNKS_V) == MB // CHUNKS_V - 1)
            def _():
                own(glv, lax.div(k, MB // CHUNKS_V))

        return 0

    lax.fori_loop(0, MB, image_tick, 0)
    def own_all(g):
        def one(q, _):
            own(g, q)
            return 0

        lax.fori_loop(0, g.pieces, one, 0)

    @pl.when(jnp.logical_not(eager))
    def _():
        ring_phase(gl5, 2)
        own_all(glv)

    ring_phase(gl5, 3)
    pair_done(gl5)
    saved_done(S5, 0)
    far_rows(S5, L5, RT, T5, R5, z5, 0, CT)
    ring_phase(glv, 1)
    ring_phase(glv, 2)
    near_rows(S5, L5, RT, d5o, CT)
    ring_phase(glv, 3)
    pair_done(glv)
    saved_done(SV, 1)
    far_rows(SV, LV, RV, TV, RV2, zv, 1, 256)
    near_rows(SV, LV, RV, dvo, 256)
    add_far(d5o, T5, R5, z5, 0, CT)
    add_far(dvo, TV, RV2, zv, 1, 256)
    @pl.when(jnp.logical_and(s >= RELAY, s < RELAY + RELAYED))
    def _():
        for kind in range(2):
            for i in range(2):
                away(0, kind, i).wait_recv()
                away(1, kind, i).start()
            for i in range(2):
                away(1, kind, i).wait_recv()
                away(2, kind, i).start()
        for kind in range(2):
            for i in range(2):
                away(1, kind, i).wait_send()
                away(2, kind, i).wait_send()

    for g in (gw5, gwv, gl5, glv):
        sent_done(g)
    for i, (ref, size) in enumerate(((s5t, RT), (svt, RV))):
        gone = ref.at[pl.ds(0, 2 * (HALF - 1) * size), :]
        pltpu.make_async_copy(gone, gone, asent.at[i]).wait()
    pltpu.make_async_copy(T5, T5, zsent.at[0]).wait()
    pltpu.make_async_copy(TV, TV, zsent.at[1]).wait()

    @pl.when(lower)
    def _():
        pltpu.make_async_copy(g5o, g5o, csent.at[0]).wait()
        pltpu.make_async_copy(gvo, gvo, csent.at[1]).wait()


def shards(vit_weight, t5_weight, vit_saved, t5_saved, vit_top_grad, t5_top_grad):
    bf, f32 = jnp.bfloat16, jnp.float32
    dma, vmem = pltpu.SemaphoreType.DMA, pl.BlockSpec(memory_space=pltpu.VMEM)
    g5, gv, d5, dv = pl.pallas_call(
        kernel,
        out_shape=(
            jax.ShapeDtypeStruct((TOK, DT), bf),
            jax.ShapeDtypeStruct((TOK, DV), bf),
            jax.ShapeDtypeStruct((RT, DT), f32),
            jax.ShapeDtypeStruct((RV, DV), f32),
        ),
        in_specs=[vmem] * 6,
        out_specs=[vmem] * 4,
        scratch_shapes=[
            pltpu.VMEM((DT, DT), bf),
            pltpu.VMEM((DV, DV), bf),
            pltpu.VMEM((HALF * TOK, DT), bf),
            pltpu.VMEM((HALF * TOK, DV), bf),
            pltpu.VMEM((2 * RT, HALF * TOK), bf),
            pltpu.VMEM((2 * RV, HALF * TOK), bf),
            pltpu.VMEM((TOK, DT), bf),
            pltpu.VMEM((TOK, DV), bf),
            pltpu.VMEM((TOK, DT), f32),
            pltpu.VMEM((TOK, DV), f32),
            pltpu.VMEM((DT, TOK), bf),
            pltpu.VMEM((DV, TOK), bf),
            pltpu.VMEM((RT, DT), bf),
            pltpu.VMEM((RV, DV), bf),
            pltpu.VMEM((RT, DT), bf),
            pltpu.VMEM((RV, DV), bf),
            pltpu.VMEM((DV, DV), bf),
            pltpu.VMEM((RT, 2 * CT), bf),
            pltpu.VMEM((RV, 512), bf),
            pltpu.VMEM((RT, 2 * CT), bf),
            pltpu.VMEM((RV, 512), bf),
            dma((2, 4, PARTS)),
            dma((2, 4, 1)),
            dma((1, 4, CHUNKS)),
            dma((1, 4, CHUNKS_V)),
            dma((4,)),
            dma((4,)),
            dma((MB, DT // CT)),
            dma((MB,)),
            dma((2,)),
            dma((2,)),
            dma((2,)),
            dma((DT // CT,)),
            dma((DV // 256,)),
            dma((2,)),
            dma((4,)),
            dma((2, 2, 2)),
            dma((2, 2, 2)),
        ],
        compiler_params=pltpu.CompilerParams(
            collective_id=0, has_side_effects=True, vmem_limit_bytes=60 * 1024 * 1024
        ),
        name="branches",
    )(
        t5_weight[0],
        vit_weight[0],
        t5_saved.reshape(TOK, DT),
        vit_saved.reshape(TOK, DV),
        t5_top_grad.reshape(TOK, DT),
        vit_top_grad.reshape(TOK, DV),
    )
    return (
        gv.reshape(vit_saved.shape),
        g5.reshape(t5_saved.shape),
        dv[None],
        d5[None],
    )


def solution(mesh):
    placed = (
        P("section", "dp", None),
        P("section", "dp", None),
        P("section", None, "dp", None),
        P("section", None, "dp", None),
        P(None, "dp", None),
        P(None, "dp", None),
    )
    return jax.shard_map(
        shards,
        mesh=mesh,
        in_specs=placed,
        out_specs=(
            P("section", None, "dp", None),
            P("section", None, "dp", None),
            P("section", "dp", None),
            P("section", "dp", None),
        ),
        check_vma=False,
    )
```

```python
import jax
import jax.numpy as jnp
from jax import lax
from jax.experimental import pallas as pl
from jax.experimental.pallas import tpu as pltpu
from jax.sharding import PartitionSpec as P

MESH = pl.DeviceIdType.MESH
root_half = 0.7071067811865476
inv_root_tau = 0.3989422804014327

SECTIONS = 16
DP = 16
DV = 1280
DT = 2048
RV = DV // DP
RT = DT // DP
TOK = 128
MICRO = 16
MB = TOK // MICRO
HALF = DP // 2
PARTS = 2
CHUNKS = 8
CHUNKS_V = 2
CT = 512
RELAYED = 2
ROW = 4
RELAY = SECTIONS - ROW
KEPT = (2, 3)
EAGER = 2
LAG = 3
EARLY = 9


def slope_of(preact):
    cumulative = 0.5 * (1.0 + lax.erf(preact * root_half))
    density = jnp.exp(-0.5 * preact * preact) * inv_root_tau
    return cumulative + preact * density


def nt(a, b):
    return lax.dot_general(a, b, (((1,), (1,)), ((), ())), preferred_element_type=jnp.float32)


def nn(a, b):
    return jnp.dot(a, b, preferred_element_type=jnp.float32)


def ds(start, size, unit):
    return pl.ds(pl.multiple_of(start, unit), size)


class Gather:
    def __init__(self, slot, part, recv, pair, sent, pieces, halves):
        self.slot, self.part, self.recv, self.pair, self.sent = slot, part, recv, pair, sent
        self.pieces, self.halves = pieces, halves


def kernel(
    w5, wv, s5_hbm, sv_hbm, top5, topv,
    g5_hbm, gv_hbm, d5_hbm, dv_hbm,
    W5, WV, L5, LV, S5, SV, G5, GV, P5, PV, s5t, svt, T5, TV, R5, RV2, WT, QT, QV, FT, FV,
    rw5, rwv, rl5, rlv, pair, sent, c5, cv, csent, asem, asent, z5, zv, zsent, lsem, rq, rsent,
    g5o, gvo, d5o, dvo, s5, sv, isem, osem,
):
    s = lax.axis_index("section")
    d = lax.axis_index("dp")
    zh = lax.div(d, 8)
    x = lax.rem(lax.div(d, 2), 4)
    c = lax.rem(d, 2)
    dr = 1 - 2 * c

    def dev(half, step, core):
        return lax.rem(zh + half, 2) * 8 + lax.rem(x + step + 8, 4) * 2 + core

    nx = dev(0, dr, c)
    zp = dev(1, 0, c)
    pt = dev(0, 0, 1 - c)
    first = s == SECTIONS - 1
    lower = s > 0
    early = s < EARLY
    eager = s < EAGER
    u = lax.rem(d, HALF)

    reads = [pltpu.make_async_copy(a, b, isem.at[i]) for i, (a, b) in enumerate(((s5_hbm, s5), (sv_hbm, sv)))]
    for copy in reads:
        copy.start()
    barrier = pltpu.get_barrier_semaphore()

    def greet(p, _):
        pl.semaphore_signal(
            barrier, inc=1, device_id=(s, lax.rem(d + p, DP)), device_id_type=MESH
        )
        return 0

    lax.fori_loop(1, DP, greet, 0)

    @pl.when(lower)
    def _():
        pl.semaphore_signal(barrier, inc=1, device_id=(s - 1, d), device_id_type=MESH)

    @pl.when(s < SECTIONS - 1)
    def _():
        pl.semaphore_signal(barrier, inc=1, device_id=(s + 1, d), device_id_type=MESH)

    W5[:, ds(d * RT, RT, RT)] = w5[...].T
    @pl.when(s < RELAYED)
    def _():
        pl.semaphore_signal(barrier, inc=1, device_id=(s + RELAY, d), device_id_type=MESH)

    @pl.when(jnp.logical_and(s >= RELAY, s < RELAY + RELAYED))
    def _():
        pl.semaphore_signal(barrier, inc=1, device_id=(s - RELAY, d), device_id_type=MESH)

    helps = jnp.logical_or(s < RELAYED, jnp.logical_and(s >= RELAY, s < RELAY + RELAYED))
    sections = helps.astype(jnp.int32)
    sections += lax.div(s + SECTIONS - 1, SECTIONS) + lax.div(2 * SECTIONS - 2 - s, SECTIONS)
    pl.semaphore_wait(barrier, DP - 1 + sections)

    gw5 = Gather(
        lambda v, q: W5.at[ds(q * (DT // PARTS), DT // PARTS, 16), ds(v * RT, RT, RT)],
        lambda n: W5.at[:, pl.ds(0, n * RT)],
        rw5, pair.at[0], sent.at[0], PARTS, 2,
    )
    gwv = Gather(
        lambda v, q: WV.at[ds(v * RV, RV, 16), :],
        lambda n: WV.at[pl.ds(0, n * RV), :],
        rwv, pair.at[1], sent.at[1], 1, 2,
    )
    piece = TOK // CHUNKS
    gl5 = Gather(
        lambda v, q: L5.at[ds(lax.rem(v, HALF) * TOK + q * piece, piece, 16), :],
        lambda n: L5.at[pl.ds(0, n * TOK), :],
        rl5, pair.at[2], sent.at[2], CHUNKS, 1,
    )
    glv = Gather(
        lambda v, q: LV.at[ds(lax.rem(v, HALF) * TOK + q * (TOK // CHUNKS_V), TOK // CHUNKS_V, 16), :],
        lambda n: LV.at[pl.ds(0, n * TOK), :],
        rlv, pair.at[3], sent.at[3], CHUNKS_V, 1,
    )

    def push(g, owner, q, recv, to):
        return pltpu.make_async_remote_copy(
            src_ref=g.slot(owner, q), dst_ref=g.slot(owner, q), send_sem=g.sent, recv_sem=recv,
            device_id=(s, to), device_id_type=MESH,
        )

    def own_ring(g, q):
        push(g, d, q, g.recv.at[0, 1, q], nx).start()

    def own_far(g, q):
        push(g, d, q, g.recv.at[1, 0, q], zp).start()

    def own_pair(g, q):
        push(g, d, q, g.pair, pt).start()

    def own(g, q):
        own_ring(g, q)
        if g.halves == 2:
            own_far(g, q)
        own_pair(g, q)

    def forward(g, h, r, q):
        owner = dev(h, -r * dr, c)
        push(g, owner, q, g.recv.at[h, r, q], nx).wait_recv()
        if r < 3:
            push(g, owner, q, g.recv.at[h, r + 1, q], nx).start()
        push(g, owner, q, g.pair, pt).start()

    def forward_when(g, h, r, q):
        @pl.when(jnp.logical_and(q >= 0, q < g.pieces))
        def _():
            forward(g, h, r, q)

    def ring_phase(g, r):
        def one(q, _):
            forward(g, 0, r, q)
            return 0

        lax.fori_loop(0, g.pieces, one, 0)

    def far_phase(g):
        def one(w, _):
            for r in range(4):
                forward_when(g, 1, r, w - r)
            return 0

        lax.fori_loop(0, g.pieces + 3, one, 0)

    def pair_done(g):
        ref = g.part(4 * g.halves)
        pltpu.make_async_copy(ref, ref, g.pair).wait()

    def sent_done(g):
        ref = g.part(8 * g.halves - 1)
        pltpu.make_async_copy(ref, ref, g.sent).wait()

    own_wv = pltpu.make_async_copy(wv, WV.at[ds(d * RV, RV, 16), :], lsem.at[0])
    own_wv.start()
    for q in range(PARTS):
        own(gw5, q)
    own_wv.wait()
    own_far(gwv, 0)
    for copy in reads:
        copy.wait()
    s5t[...] = s5[...].T
    svt[...] = sv[...].T

    def saved_rows(h, v):
        text = s5t.at[ds(v * RT, RT, RT), :], S5.at[pl.ds(h * RT, RT), ds(u * TOK, TOK, TOK)]
        image = svt.at[ds(v * RV, RV, 16), :], SV.at[pl.ds(h * RV, RV), ds(u * TOK, TOK, TOK)]
        return text, image

    stay = []
    for h, v in ((0, d), (1, zp)):
        for i, (src, dst) in enumerate(saved_rows(h, v)):
            stay.append(pltpu.make_async_copy(src, dst, lsem.at[2 * h + i]))
    for copy in stay:
        copy.start()
    for copy in stay:
        copy.wait()

    @pl.when(first)
    def _():
        for k in range(MB):
            rows = pl.ds(k * MICRO, MICRO)
            for n in range(DT // CT):
                cols = pl.ds(n * CT, CT)
                pltpu.make_async_copy(top5.at[rows, cols], G5.at[rows, cols], c5.at[k, n]).start()
            pltpu.make_async_copy(topv.at[rows, :], GV.at[rows, :], cv.at[k]).start()

    for r in (1, 2, 3):
        ring_phase(gw5, r)
    far_phase(gw5)
    own_ring(gwv, 0)
    own_pair(gwv, 0)
    pair_done(gw5)

    def text_slope(j, _):
        cols = ds(j * CT, CT, CT)
        P5[:, cols] = slope_of(nt(s5[...], W5[cols, :]))
        return 0

    lax.fori_loop(0, DT // CT, text_slope, 0)

    image_steps = ((1, 0), (0, 1), (1, 1), (0, 2), (1, 2), (0, 3), (1, 3))

    def image_ready():
        pair_done(gwv)
        WT[...] = WV[...].T

        def one(j, _):
            cols = ds(j * 256, 256, 256)
            PV[:, cols] = slope_of(nn(sv[...], WV[:, cols]))
            return 0

        lax.fori_loop(0, DV // 256, one, 0)

        def send(p, _):
            up = lax.rem(u + p, HALF)
            t = zh * HALF + up
            for h, v in ((0, t), (1, (1 - zh) * HALF + up)):
                for i, (src, dst) in enumerate(saved_rows(h, v)):
                    pltpu.make_async_remote_copy(
                        src_ref=src, dst_ref=dst, send_sem=asent.at[i], recv_sem=asem.at[i],
                        device_id=(s, t), device_id_type=MESH,
                    ).start()
            return 0

        lax.fori_loop(1, HALF, send, 0)

    @pl.when(early)
    def _():
        for h, r in image_steps:
            forward(gwv, h, r, 0)
        image_ready()

    def text_hop(k, n):
        rows, cols = ds(k * MICRO, MICRO, MICRO), pl.ds(n * CT, CT)
        return pltpu.make_async_remote_copy(
            src_ref=g5o.at[rows, cols], dst_ref=G5.at[rows, cols], send_sem=csent.at[0], recv_sem=c5.at[k, n],
            device_id=(s - 1, d), device_id_type=MESH,
        )

    def text_tick(sends):
        def tick(k, _):
            rows = ds(k * MICRO, MICRO, MICRO)
            pieces = [pl.ds(n * CT, CT) for n in range(DT // CT)]
            total = [None] * len(pieces)
            for m, inner in enumerate(pieces):
                text_hop(k, m).wait_recv()
                local = (G5[rows, inner].astype(jnp.float32) * P5[rows, inner]).astype(jnp.bfloat16)
                L5[ds(u * TOK + k * MICRO, MICRO, MICRO), inner] = local
                for n, cols in enumerate(pieces):
                    term = nn(local, W5[inner, cols])
                    total[n] = term if m == 0 else total[n] + term
                    if m == len(pieces) - 1:
                        above = G5[rows, cols].astype(jnp.float32)
                        g5o[rows, cols] = (above + total[n]).astype(jnp.bfloat16)
                        if sends:
                            text_hop(k, n).start()

            own(gl5, k)

            @pl.when(eager)
            def _():
                forward_when(gl5, 0, 1, k - LAG)

            @pl.when(jnp.logical_not(early))
            def _():
                for i, (h, r) in enumerate(image_steps):

                    @pl.when(k == i)
                    def _():
                        forward(gwv, h, r, 0)

            return 0

        lax.fori_loop(0, MB, tick, 0)

    @pl.when(lower)
    def _():
        text_tick(True)

    @pl.when(jnp.logical_not(lower))
    def _():
        text_tick(False)

    @pl.when(jnp.logical_not(early))
    def _():
        image_ready()

    def image_hop(k):
        rows = ds(k * MICRO, MICRO, MICRO)
        return pltpu.make_async_remote_copy(
            src_ref=gvo.at[rows, :], dst_ref=GV.at[rows, :], send_sem=csent.at[1], recv_sem=cv.at[k],
            device_id=(s - 1, d), device_id_type=MESH,
        )

    def exchange(out, got, recv, sem, n, width):
        cols = ds(n * width, width, width)
        return pltpu.make_async_remote_copy(
            src_ref=out.at[:, cols], dst_ref=got.at[:, cols], send_sem=zsent.at[sem], recv_sem=recv.at[n],
            device_id=(s, zp), device_id_type=MESH,
        )

    def away(stage, kind, i):
        width = (CT, 256)[kind]
        here, there = pl.ds(i * width, width), pl.ds((i + KEPT[kind]) * width, width)
        out, first_stop, second_stop, got = ((T5, QT, FT, R5), (TV, QV, FV, RV2))[kind]
        src = (out.at[:, there], first_stop.at[:, here], second_stop.at[:, here])[stage]
        dst = (first_stop.at[:, here], second_stop.at[:, here], got.at[:, there])[stage]
        recv = rq.at[stage, kind, i] if stage < 2 else (z5, zv)[kind].at[i + KEPT[kind]]
        to = ((s + RELAY, d), (s, zp), (s - RELAY, d))[stage]
        return pltpu.make_async_remote_copy(
            src_ref=src, dst_ref=dst, send_sem=zsent.at[kind] if stage == 0 else rsent.at[stage - 1, kind, i],
            recv_sem=recv, device_id=to, device_id_type=MESH,
        )

    def far_rows(saved, local, rows, out, got, recv, sem, width):
        def one(n, _):
            cols = ds(n * width, width, width)
            term = nn(saved[pl.ds(rows, rows), :], local[:, cols]) * (1.0 / TOK)
            out[:, cols] = term.astype(jnp.bfloat16)
            far = jnp.logical_and(s < RELAYED, n >= KEPT[sem])

            @pl.when(jnp.logical_not(far))
            def _():
                exchange(out, got, recv, sem, n, width).start()

            for i in range(2):

                @pl.when(jnp.logical_and(far, n == i + KEPT[sem]))
                def _():
                    away(0, sem, i).start()

            return 0

        lax.fori_loop(0, local.shape[1] // width, one, 0)

    def near_rows(saved, local, rows, total, width):
        def one(n, _):
            cols = ds(n * width, width, width)
            total[:, cols] = nn(saved[pl.ds(0, rows), :], local[:, cols]) * (1.0 / TOK)
            return 0

        lax.fori_loop(0, local.shape[1] // width, one, 0)

    def put(total, n, width, hbm, sem):
        cols = ds(n * width, width, width)
        return pltpu.make_async_copy(total.at[:, cols], hbm.at[:, cols], osem.at[sem])

    def add_far(total, out, got, recv, sem, width, hbm):
        def one(n, _):
            cols = ds(n * width, width, width)
            exchange(out, got, recv, sem, n, width).wait_recv()
            total[:, cols] += got[:, cols].astype(jnp.float32)
            put(total, n, width, hbm, sem).start()
            return 0

        lax.fori_loop(0, total.shape[1] // width, one, 0)

    def saved_done(ref, i):
        got = ref.at[:, pl.ds(0, (HALF - 1) * TOK)]
        pltpu.make_async_copy(got, got, asem.at[i]).wait()

    def image_tick(k, _):
        rows = ds(k * MICRO, MICRO, MICRO)
        image_hop(k).wait_recv()
        upper = GV[rows, :].astype(jnp.float32)
        local = (upper * PV[rows, :]).astype(jnp.bfloat16)
        LV[ds(u * TOK + k * MICRO, MICRO, MICRO), :] = local
        gvo[rows, :] = (upper + nn(local, WT[...])).astype(jnp.bfloat16)

        @pl.when(lower)
        def _():
            image_hop(k).start()


        @pl.when(jnp.logical_or(jnp.logical_not(eager), k < LAG))
        def _():
            forward(gl5, 0, 1, k + jnp.where(eager, MB - LAG, 0))

        @pl.when(eager)
        def _():
            forward(gl5, 0, 2, k)

            @pl.when(lax.rem(k, MB // CHUNKS_V) == MB // CHUNKS_V - 1)
            def _():
                own(glv, lax.div(k, MB // CHUNKS_V))

        return 0

    lax.fori_loop(0, MB, image_tick, 0)
    writes = [pltpu.make_async_copy(a, b, osem.at[2 + i]) for i, (a, b) in enumerate(((g5o, g5_hbm), (gvo, gv_hbm)))]
    for copy in writes:
        copy.start()
    def own_all(g):
        def one(q, _):
            own(g, q)
            return 0

        lax.fori_loop(0, g.pieces, one, 0)

    @pl.when(jnp.logical_not(eager))
    def _():
        ring_phase(gl5, 2)
        own_all(glv)

    ring_phase(gl5, 3)
    pair_done(gl5)
    saved_done(S5, 0)
    far_rows(S5, L5, RT, T5, R5, z5, 0, CT)
    ring_phase(glv, 1)
    ring_phase(glv, 2)
    near_rows(S5, L5, RT, d5o, CT)
    ring_phase(glv, 3)
    pair_done(glv)
    saved_done(SV, 1)
    far_rows(SV, LV, RV, TV, RV2, zv, 1, 256)
    near_rows(SV, LV, RV, dvo, 256)
    add_far(d5o, T5, R5, z5, 0, CT, d5_hbm)
    add_far(dvo, TV, RV2, zv, 1, 256, dv_hbm)
    @pl.when(jnp.logical_and(s >= RELAY, s < RELAY + RELAYED))
    def _():
        for kind in range(2):
            for i in range(2):
                away(0, kind, i).wait_recv()
                away(1, kind, i).start()
            for i in range(2):
                away(1, kind, i).wait_recv()
                away(2, kind, i).start()
        for kind in range(2):
            for i in range(2):
                away(1, kind, i).wait_send()
                away(2, kind, i).wait_send()

    for g in (gw5, gwv, gl5, glv):
        sent_done(g)
    for copy in writes:
        copy.wait()
    pltpu.make_async_copy(d5o, d5_hbm, osem.at[0]).wait()
    pltpu.make_async_copy(dvo, dv_hbm, osem.at[1]).wait()
    for i, (ref, size) in enumerate(((s5t, RT), (svt, RV))):
        gone = ref.at[pl.ds(0, 2 * (HALF - 1) * size), :]
        pltpu.make_async_copy(gone, gone, asent.at[i]).wait()
    pltpu.make_async_copy(T5, T5, zsent.at[0]).wait()
    pltpu.make_async_copy(TV, TV, zsent.at[1]).wait()

    @pl.when(lower)
    def _():
        pltpu.make_async_copy(g5o, g5o, csent.at[0]).wait()
        pltpu.make_async_copy(gvo, gvo, csent.at[1]).wait()


def hand_over(*refs):
    given, out, held, came, went = refs[:4], refs[4:8], refs[8:12], refs[12], refs[13]
    reads = [pltpu.make_async_copy(a, b, came.at[i]) for i, (a, b) in enumerate(zip(given, held))]
    writes = [pltpu.make_async_copy(a, b, went.at[i]) for i, (a, b) in enumerate(zip(held, out))]
    for copy in reads:
        copy.start()
    for read, write in zip(reads, writes):
        read.wait()
        write.start()
    for copy in writes:
        copy.wait()


def shards(vit_weight, t5_weight, vit_saved, t5_saved, vit_top_grad, t5_top_grad):
    bf, f32 = jnp.bfloat16, jnp.float32
    dma, vmem = pltpu.SemaphoreType.DMA, pl.BlockSpec(memory_space=pltpu.VMEM)
    hbm = pl.BlockSpec(memory_space=pl.ANY)
    g5, gv, d5, dv = pl.pallas_call(
        kernel,
        out_shape=(
            jax.ShapeDtypeStruct((TOK, DT), bf),
            jax.ShapeDtypeStruct((TOK, DV), bf),
            jax.ShapeDtypeStruct((RT, DT), f32),
            jax.ShapeDtypeStruct((RV, DV), f32),
        ),
        in_specs=[vmem, vmem, hbm, hbm, hbm, hbm],
        out_specs=[hbm] * 4,
        scratch_shapes=[
            pltpu.VMEM((DT, DT), bf),
            pltpu.VMEM((DV, DV), bf),
            pltpu.VMEM((HALF * TOK, DT), bf),
            pltpu.VMEM((HALF * TOK, DV), bf),
            pltpu.VMEM((2 * RT, HALF * TOK), bf),
            pltpu.VMEM((2 * RV, HALF * TOK), bf),
            pltpu.VMEM((TOK, DT), bf),
            pltpu.VMEM((TOK, DV), bf),
            pltpu.VMEM((TOK, DT), f32),
            pltpu.VMEM((TOK, DV), f32),
            pltpu.VMEM((DT, TOK), bf),
            pltpu.VMEM((DV, TOK), bf),
            pltpu.VMEM((RT, DT), bf),
            pltpu.VMEM((RV, DV), bf),
            pltpu.VMEM((RT, DT), bf),
            pltpu.VMEM((RV, DV), bf),
            pltpu.VMEM((DV, DV), bf),
            pltpu.VMEM((RT, 2 * CT), bf),
            pltpu.VMEM((RV, 512), bf),
            pltpu.VMEM((RT, 2 * CT), bf),
            pltpu.VMEM((RV, 512), bf),
            dma((2, 4, PARTS)),
            dma((2, 4, 1)),
            dma((1, 4, CHUNKS)),
            dma((1, 4, CHUNKS_V)),
            dma((4,)),
            dma((4,)),
            dma((MB, DT // CT)),
            dma((MB,)),
            dma((2,)),
            dma((2,)),
            dma((2,)),
            dma((DT // CT,)),
            dma((DV // 256,)),
            dma((2,)),
            dma((4,)),
            dma((2, 2, 2)),
            dma((2, 2, 2)),
            pltpu.VMEM((TOK, DT), bf),
            pltpu.VMEM((TOK, DV), bf),
            pltpu.VMEM((RT, DT), f32),
            pltpu.VMEM((RV, DV), f32),
            pltpu.VMEM((TOK, DT), bf),
            pltpu.VMEM((TOK, DV), bf),
            dma((2,)),
            dma((4,)),
        ],
        compiler_params=pltpu.CompilerParams(
            collective_id=0, has_side_effects=True, vmem_limit_bytes=60 * 1024 * 1024
        ),
        name="branches",
    )(
        t5_weight[0],
        vit_weight[0],
        t5_saved.reshape(TOK, DT),
        vit_saved.reshape(TOK, DV),
        t5_top_grad.reshape(TOK, DT),
        vit_top_grad.reshape(TOK, DV),
    )
    gv, g5, dv, d5 = pl.pallas_call(
        hand_over,
        out_shape=tuple(jax.ShapeDtypeStruct(a.shape, a.dtype) for a in (gv, g5, dv, d5)),
        in_specs=[hbm] * 4,
        out_specs=[hbm] * 4,
        scratch_shapes=[pltpu.VMEM(a.shape, a.dtype) for a in (gv, g5, dv, d5)] + [dma((4,)), dma((4,))],
        name="hand_over",
    )(gv, g5, dv, d5)
    return (
        gv.reshape(vit_saved.shape),
        g5.reshape(t5_saved.shape),
        dv[None],
        d5[None],
    )


def solution(mesh):
    placed = (
        P("section", "dp", None),
        P("section", "dp", None),
        P("section", None, "dp", None),
        P("section", None, "dp", None),
        P(None, "dp", None),
        P(None, "dp", None),
    )
    return jax.shard_map(
        shards,
        mesh=mesh,
        in_specs=placed,
        out_specs=(
            P("section", None, "dp", None),
            P("section", None, "dp", None),
            P("section", "dp", None),
            P("section", "dp", None),
        ),
        check_vma=False,
    )
```

```python
import jax
import jax.numpy as jnp
from jax import lax
from jax.experimental import pallas as pl
from jax.experimental.pallas import tpu as pltpu
from jax.sharding import PartitionSpec as P

MESH = pl.DeviceIdType.MESH
root_half = 0.7071067811865476
inv_root_tau = 0.3989422804014327

SECTIONS = 16
DP = 16
DV = 1280
DT = 2048
RV = DV // DP
RT = DT // DP
TOK = 128
MICRO = 16
MB = TOK // MICRO
HALF = DP // 2
PARTS = 2
CHUNKS = 8
CHUNKS_V = 2
CT = 512
RELAYED = 2
ROW = 4
RELAY = SECTIONS - ROW
KEPT = (2, 3)
EAGER = 2
LAG = 3
EARLY = 9


def slope_of(preact):
    cumulative = 0.5 * (1.0 + lax.erf(preact * root_half))
    density = jnp.exp(-0.5 * preact * preact) * inv_root_tau
    return cumulative + preact * density


def nt(a, b):
    return lax.dot_general(a, b, (((1,), (1,)), ((), ())), preferred_element_type=jnp.float32)


def nn(a, b):
    return jnp.dot(a, b, preferred_element_type=jnp.float32)


def ds(start, size, unit):
    return pl.ds(pl.multiple_of(start, unit), size)


class Gather:
    def __init__(self, slot, part, recv, pair, sent, pieces, halves):
        self.slot, self.part, self.recv, self.pair, self.sent = slot, part, recv, pair, sent
        self.pieces, self.halves = pieces, halves


def kernel(
    w5, wv, s5_hbm, sv_hbm, top5, topv,
    g5_hbm, gv_hbm, d5_hbm, dv_hbm,
    W5, WV, L5, LV, S5, SV, G5, GV, P5, PV, s5t, svt, T5, TV, R5, RV2, WT, QT, QV, FT, FV,
    rw5, rwv, rl5, rlv, pair, sent, c5, cv, csent, asem, asent, z5, zv, zsent, lsem, rq, rsent,
    g5o, gvo, d5o, dvo, s5, sv, isem, osem,
):
    s = lax.axis_index("section")
    d = lax.axis_index("dp")
    zh = lax.div(d, 8)
    x = lax.rem(lax.div(d, 2), 4)
    c = lax.rem(d, 2)
    dr = 1 - 2 * c

    def dev(half, step, core):
        return lax.rem(zh + half, 2) * 8 + lax.rem(x + step + 8, 4) * 2 + core

    nx = dev(0, dr, c)
    zp = dev(1, 0, c)
    pt = dev(0, 0, 1 - c)
    first = s == SECTIONS - 1
    lower = s > 0
    early = s < EARLY
    eager = s < EAGER
    u = lax.rem(d, HALF)

    reads = [pltpu.make_async_copy(a, b, isem.at[i]) for i, (a, b) in enumerate(((s5_hbm, s5), (sv_hbm, sv)))]
    for copy in reads:
        copy.start()
    barrier = pltpu.get_barrier_semaphore()

    def greet(p, _):
        pl.semaphore_signal(
            barrier, inc=1, device_id=(s, lax.rem(d + p, DP)), device_id_type=MESH
        )
        return 0

    lax.fori_loop(1, DP, greet, 0)

    @pl.when(lower)
    def _():
        pl.semaphore_signal(barrier, inc=1, device_id=(s - 1, d), device_id_type=MESH)

    @pl.when(s < SECTIONS - 1)
    def _():
        pl.semaphore_signal(barrier, inc=1, device_id=(s + 1, d), device_id_type=MESH)

    W5[:, ds(d * RT, RT, RT)] = w5[...].T
    @pl.when(s < RELAYED)
    def _():
        pl.semaphore_signal(barrier, inc=1, device_id=(s + RELAY, d), device_id_type=MESH)

    @pl.when(jnp.logical_and(s >= RELAY, s < RELAY + RELAYED))
    def _():
        pl.semaphore_signal(barrier, inc=1, device_id=(s - RELAY, d), device_id_type=MESH)

    helps = jnp.logical_or(s < RELAYED, jnp.logical_and(s >= RELAY, s < RELAY + RELAYED))
    sections = helps.astype(jnp.int32)
    sections += lax.div(s + SECTIONS - 1, SECTIONS) + lax.div(2 * SECTIONS - 2 - s, SECTIONS)
    pl.semaphore_wait(barrier, DP - 1 + sections)

    gw5 = Gather(
        lambda v, q: W5.at[ds(q * (DT // PARTS), DT // PARTS, 16), ds(v * RT, RT, RT)],
        lambda n: W5.at[:, pl.ds(0, n * RT)],
        rw5, pair.at[0], sent.at[0], PARTS, 2,
    )
    gwv = Gather(
        lambda v, q: WV.at[ds(v * RV, RV, 16), :],
        lambda n: WV.at[pl.ds(0, n * RV), :],
        rwv, pair.at[1], sent.at[1], 1, 2,
    )
    piece = TOK // CHUNKS
    gl5 = Gather(
        lambda v, q: L5.at[ds(lax.rem(v, HALF) * TOK + q * piece, piece, 16), :],
        lambda n: L5.at[pl.ds(0, n * TOK), :],
        rl5, pair.at[2], sent.at[2], CHUNKS, 1,
    )
    glv = Gather(
        lambda v, q: LV.at[ds(lax.rem(v, HALF) * TOK + q * (TOK // CHUNKS_V), TOK // CHUNKS_V, 16), :],
        lambda n: LV.at[pl.ds(0, n * TOK), :],
        rlv, pair.at[3], sent.at[3], CHUNKS_V, 1,
    )

    def push(g, owner, q, recv, to):
        return pltpu.make_async_remote_copy(
            src_ref=g.slot(owner, q), dst_ref=g.slot(owner, q), send_sem=g.sent, recv_sem=recv,
            device_id=(s, to), device_id_type=MESH,
        )

    def own_ring(g, q):
        push(g, d, q, g.recv.at[0, 1, q], nx).start()

    def own_far(g, q):
        push(g, d, q, g.recv.at[1, 0, q], zp).start()

    def own_pair(g, q):
        push(g, d, q, g.pair, pt).start()

    def own(g, q):
        own_ring(g, q)
        if g.halves == 2:
            own_far(g, q)
        own_pair(g, q)

    def forward(g, h, r, q):
        owner = dev(h, -r * dr, c)
        push(g, owner, q, g.recv.at[h, r, q], nx).wait_recv()
        if r < 3:
            push(g, owner, q, g.recv.at[h, r + 1, q], nx).start()
        push(g, owner, q, pair.at[4] if g is gw5 and h == 1 else g.pair, pt).start()

    def forward_when(g, h, r, q):
        @pl.when(jnp.logical_and(q >= 0, q < g.pieces))
        def _():
            forward(g, h, r, q)

    def ring_phase(g, r):
        def one(q, _):
            forward(g, 0, r, q)
            return 0

        lax.fori_loop(0, g.pieces, one, 0)

    def far_phase(g, begin=0, end=None):
        def one(w, _):
            for r in range(4):
                forward_when(g, 1, r, w - r)
            return 0

        lax.fori_loop(begin, g.pieces + 3 if end is None else end, one, 0)

    def pair_done(g):
        ref = g.part(4 * g.halves)
        pltpu.make_async_copy(ref, ref, g.pair).wait()

    def sent_done(g):
        ref = g.part(8 * g.halves - 1)
        pltpu.make_async_copy(ref, ref, g.sent).wait()

    own_wv = pltpu.make_async_copy(wv, WV.at[ds(d * RV, RV, 16), :], lsem.at[0])
    own_wv.start()
    for q in range(PARTS):
        own(gw5, q)
    own_wv.wait()
    own_far(gwv, 0)
    for copy in reads:
        copy.wait()
    s5t[...] = s5[...].T
    svt[...] = sv[...].T

    def saved_rows(h, v):
        text = s5t.at[ds(v * RT, RT, RT), :], S5.at[pl.ds(h * RT, RT), ds(u * TOK, TOK, TOK)]
        image = svt.at[ds(v * RV, RV, 16), :], SV.at[pl.ds(h * RV, RV), ds(u * TOK, TOK, TOK)]
        return text, image

    stay = []
    for h, v in ((0, d), (1, zp)):
        for i, (src, dst) in enumerate(saved_rows(h, v)):
            stay.append(pltpu.make_async_copy(src, dst, lsem.at[2 * h + i]))
    for copy in stay:
        copy.start()
    for copy in stay:
        copy.wait()

    @pl.when(first)
    def _():
        for k in range(MB):
            rows = pl.ds(k * MICRO, MICRO)
            for n in range(DT // CT):
                cols = pl.ds(n * CT, CT)
                pltpu.make_async_copy(top5.at[rows, cols], G5.at[rows, cols], c5.at[k, n]).start()
            pltpu.make_async_copy(topv.at[rows, :], GV.at[rows, :], cv.at[k]).start()

    for r in (1, 2, 3):
        ring_phase(gw5, r)
    far_phase(gw5, 0, 1)
    share = gw5.part(4)
    pltpu.make_async_copy(share, share, gw5.pair).wait()
    near = ds(zh * (DT // 2), DT // 2, DT // 2)
    far_half = ds((1 - zh) * (DT // 2), DT // 2, DT // 2)

    def text_near(j, _):
        cols = ds(j * CT, CT, CT)
        P5[:, cols] = nt(s5[:, near], W5[cols, near])
        return 0

    lax.fori_loop(0, DT // CT, text_near, 0)
    far_phase(gw5, 1)
    own_ring(gwv, 0)
    own_pair(gwv, 0)
    pltpu.make_async_copy(share, share, pair.at[4]).wait()

    def text_slope(j, _):
        cols = ds(j * CT, CT, CT)
        P5[:, cols] = slope_of(P5[:, cols] + nt(s5[:, far_half], W5[cols, far_half]))
        return 0

    lax.fori_loop(0, DT // CT, text_slope, 0)

    image_steps = ((1, 0), (0, 1), (1, 1), (0, 2), (1, 2), (0, 3), (1, 3))

    def image_ready():
        pair_done(gwv)
        WT[...] = WV[...].T

        def one(j, _):
            cols = ds(j * 256, 256, 256)
            PV[:, cols] = slope_of(nn(sv[...], WV[:, cols]))
            return 0

        lax.fori_loop(0, DV // 256, one, 0)

        def send(p, _):
            up = lax.rem(u + p, HALF)
            t = zh * HALF + up
            for h, v in ((0, t), (1, (1 - zh) * HALF + up)):
                for i, (src, dst) in enumerate(saved_rows(h, v)):
                    pltpu.make_async_remote_copy(
                        src_ref=src, dst_ref=dst, send_sem=asent.at[i], recv_sem=asem.at[i],
                        device_id=(s, t), device_id_type=MESH,
                    ).start()
            return 0

        lax.fori_loop(1, HALF, send, 0)

    @pl.when(early)
    def _():
        for h, r in image_steps:
            forward(gwv, h, r, 0)
        image_ready()

    def text_hop(k, n):
        rows, cols = ds(k * MICRO, MICRO, MICRO), pl.ds(n * CT, CT)
        return pltpu.make_async_remote_copy(
            src_ref=g5o.at[rows, cols], dst_ref=G5.at[rows, cols], send_sem=csent.at[0], recv_sem=c5.at[k, n],
            device_id=(s - 1, d), device_id_type=MESH,
        )

    def text_tick(sends):
        def tick(k, _):
            rows = ds(k * MICRO, MICRO, MICRO)
            pieces = [pl.ds(n * CT, CT) for n in range(DT // CT)]
            total = [None] * len(pieces)
            for m, inner in enumerate(pieces):
                text_hop(k, m).wait_recv()
                local = (G5[rows, inner].astype(jnp.float32) * P5[rows, inner]).astype(jnp.bfloat16)
                L5[ds(u * TOK + k * MICRO, MICRO, MICRO), inner] = local
                for n, cols in enumerate(pieces):
                    term = nn(local, W5[inner, cols])
                    total[n] = term if m == 0 else total[n] + term
                    if m == len(pieces) - 1:
                        above = G5[rows, cols].astype(jnp.float32)
                        g5o[rows, cols] = (above + total[n]).astype(jnp.bfloat16)
                        if sends:
                            text_hop(k, n).start()

            own(gl5, k)

            @pl.when(eager)
            def _():
                forward_when(gl5, 0, 1, k - LAG)

            @pl.when(jnp.logical_not(early))
            def _():
                for i, (h, r) in enumerate(image_steps):

                    @pl.when(k == i)
                    def _():
                        forward(gwv, h, r, 0)

            return 0

        lax.fori_loop(0, MB, tick, 0)

    @pl.when(lower)
    def _():
        text_tick(True)

    @pl.when(jnp.logical_not(lower))
    def _():
        text_tick(False)

    @pl.when(jnp.logical_not(early))
    def _():
        image_ready()

    def image_hop(k):
        rows = ds(k * MICRO, MICRO, MICRO)
        return pltpu.make_async_remote_copy(
            src_ref=gvo.at[rows, :], dst_ref=GV.at[rows, :], send_sem=csent.at[1], recv_sem=cv.at[k],
            device_id=(s - 1, d), device_id_type=MESH,
        )

    def exchange(out, got, recv, sem, n, width):
        cols = ds(n * width, width, width)
        return pltpu.make_async_remote_copy(
            src_ref=out.at[:, cols], dst_ref=got.at[:, cols], send_sem=zsent.at[sem], recv_sem=recv.at[n],
            device_id=(s, zp), device_id_type=MESH,
        )

    def away(stage, kind, i):
        width = (CT, 256)[kind]
        here, there = pl.ds(i * width, width), pl.ds((i + KEPT[kind]) * width, width)
        out, first_stop, second_stop, got = ((T5, QT, FT, R5), (TV, QV, FV, RV2))[kind]
        src = (out.at[:, there], first_stop.at[:, here], second_stop.at[:, here])[stage]
        dst = (first_stop.at[:, here], second_stop.at[:, here], got.at[:, there])[stage]
        recv = rq.at[stage, kind, i] if stage < 2 else (z5, zv)[kind].at[i + KEPT[kind]]
        to = ((s + RELAY, d), (s, zp), (s - RELAY, d))[stage]
        return pltpu.make_async_remote_copy(
            src_ref=src, dst_ref=dst, send_sem=zsent.at[kind] if stage == 0 else rsent.at[stage - 1, kind, i],
            recv_sem=recv, device_id=to, device_id_type=MESH,
        )

    def far_rows(saved, local, rows, out, got, recv, sem, width):
        def one(n, _):
            cols = ds(n * width, width, width)
            term = nn(saved[pl.ds(rows, rows), :], local[:, cols]) * (1.0 / TOK)
            out[:, cols] = term.astype(jnp.bfloat16)
            far = jnp.logical_and(s < RELAYED, n >= KEPT[sem])

            @pl.when(jnp.logical_not(far))
            def _():
                exchange(out, got, recv, sem, n, width).start()

            for i in range(2):

                @pl.when(jnp.logical_and(far, n == i + KEPT[sem]))
                def _():
                    away(0, sem, i).start()

            return 0

        lax.fori_loop(0, local.shape[1] // width, one, 0)

    def near_rows(saved, local, rows, total, width):
        def one(n, _):
            cols = ds(n * width, width, width)
            total[:, cols] = nn(saved[pl.ds(0, rows), :], local[:, cols]) * (1.0 / TOK)
            return 0

        lax.fori_loop(0, local.shape[1] // width, one, 0)

    def put(total, n, width, hbm, sem):
        cols = ds(n * width, width, width)
        return pltpu.make_async_copy(total.at[:, cols], hbm.at[:, cols], osem.at[sem])

    def add_far(total, out, got, recv, sem, width, hbm):
        def one(n, _):
            cols = ds(n * width, width, width)
            exchange(out, got, recv, sem, n, width).wait_recv()
            total[:, cols] += got[:, cols].astype(jnp.float32)
            put(total, n, width, hbm, sem).start()
            return 0

        lax.fori_loop(0, total.shape[1] // width, one, 0)

    def saved_done(ref, i):
        got = ref.at[:, pl.ds(0, (HALF - 1) * TOK)]
        pltpu.make_async_copy(got, got, asem.at[i]).wait()

    def image_tick(k, _):
        rows = ds(k * MICRO, MICRO, MICRO)
        image_hop(k).wait_recv()
        upper = GV[rows, :].astype(jnp.float32)
        local = (upper * PV[rows, :]).astype(jnp.bfloat16)
        LV[ds(u * TOK + k * MICRO, MICRO, MICRO), :] = local
        gvo[rows, :] = (upper + nn(local, WT[...])).astype(jnp.bfloat16)

        @pl.when(lower)
        def _():
            image_hop(k).start()


        @pl.when(jnp.logical_or(jnp.logical_not(eager), k < LAG))
        def _():
            forward(gl5, 0, 1, k + jnp.where(eager, MB - LAG, 0))

        @pl.when(eager)
        def _():
            forward(gl5, 0, 2, k)

            @pl.when(lax.rem(k, MB // CHUNKS_V) == MB // CHUNKS_V - 1)
            def _():
                own(glv, lax.div(k, MB // CHUNKS_V))

        return 0

    lax.fori_loop(0, MB, image_tick, 0)
    writes = [pltpu.make_async_copy(a, b, osem.at[2 + i]) for i, (a, b) in enumerate(((g5o, g5_hbm), (gvo, gv_hbm)))]
    for copy in writes:
        copy.start()
    def own_all(g):
        def one(q, _):
            own(g, q)
            return 0

        lax.fori_loop(0, g.pieces, one, 0)

    @pl.when(jnp.logical_not(eager))
    def _():
        ring_phase(gl5, 2)
        own_all(glv)

    ring_phase(gl5, 3)
    pair_done(gl5)
    saved_done(S5, 0)
    far_rows(S5, L5, RT, T5, R5, z5, 0, CT)
    ring_phase(glv, 1)
    ring_phase(glv, 2)
    near_rows(S5, L5, RT, d5o, CT)
    ring_phase(glv, 3)
    pair_done(glv)
    saved_done(SV, 1)
    far_rows(SV, LV, RV, TV, RV2, zv, 1, 256)
    near_rows(SV, LV, RV, dvo, 256)
    add_far(d5o, T5, R5, z5, 0, CT, d5_hbm)
    add_far(dvo, TV, RV2, zv, 1, 256, dv_hbm)
    @pl.when(jnp.logical_and(s >= RELAY, s < RELAY + RELAYED))
    def _():
        for kind in range(2):
            for i in range(2):
                away(0, kind, i).wait_recv()
                away(1, kind, i).start()
            for i in range(2):
                away(1, kind, i).wait_recv()
                away(2, kind, i).start()
        for kind in range(2):
            for i in range(2):
                away(1, kind, i).wait_send()
                away(2, kind, i).wait_send()

    for g in (gw5, gwv, gl5, glv):
        sent_done(g)
    for copy in writes:
        copy.wait()
    pltpu.make_async_copy(d5o, d5_hbm, osem.at[0]).wait()
    pltpu.make_async_copy(dvo, dv_hbm, osem.at[1]).wait()
    for i, (ref, size) in enumerate(((s5t, RT), (svt, RV))):
        gone = ref.at[pl.ds(0, 2 * (HALF - 1) * size), :]
        pltpu.make_async_copy(gone, gone, asent.at[i]).wait()
    pltpu.make_async_copy(T5, T5, zsent.at[0]).wait()
    pltpu.make_async_copy(TV, TV, zsent.at[1]).wait()

    @pl.when(lower)
    def _():
        pltpu.make_async_copy(g5o, g5o, csent.at[0]).wait()
        pltpu.make_async_copy(gvo, gvo, csent.at[1]).wait()


def hand_over(*refs):
    given, out, held, came, went = refs[:4], refs[4:8], refs[8:12], refs[12], refs[13]
    reads = [pltpu.make_async_copy(a, b, came.at[i]) for i, (a, b) in enumerate(zip(given, held))]
    writes = [pltpu.make_async_copy(a, b, went.at[i]) for i, (a, b) in enumerate(zip(held, out))]
    for copy in reads:
        copy.start()
    for read, write in zip(reads, writes):
        read.wait()
        write.start()
    for copy in writes:
        copy.wait()


def shards(vit_weight, t5_weight, vit_saved, t5_saved, vit_top_grad, t5_top_grad):
    bf, f32 = jnp.bfloat16, jnp.float32
    dma, vmem = pltpu.SemaphoreType.DMA, pl.BlockSpec(memory_space=pltpu.VMEM)
    hbm = pl.BlockSpec(memory_space=pl.ANY)
    g5, gv, d5, dv = pl.pallas_call(
        kernel,
        out_shape=(
            jax.ShapeDtypeStruct((TOK, DT), bf),
            jax.ShapeDtypeStruct((TOK, DV), bf),
            jax.ShapeDtypeStruct((RT, DT), f32),
            jax.ShapeDtypeStruct((RV, DV), f32),
        ),
        in_specs=[vmem, vmem, hbm, hbm, hbm, hbm],
        out_specs=[hbm] * 4,
        scratch_shapes=[
            pltpu.VMEM((DT, DT), bf),
            pltpu.VMEM((DV, DV), bf),
            pltpu.VMEM((HALF * TOK, DT), bf),
            pltpu.VMEM((HALF * TOK, DV), bf),
            pltpu.VMEM((2 * RT, HALF * TOK), bf),
            pltpu.VMEM((2 * RV, HALF * TOK), bf),
            pltpu.VMEM((TOK, DT), bf),
            pltpu.VMEM((TOK, DV), bf),
            pltpu.VMEM((TOK, DT), f32),
            pltpu.VMEM((TOK, DV), f32),
            pltpu.VMEM((DT, TOK), bf),
            pltpu.VMEM((DV, TOK), bf),
            pltpu.VMEM((RT, DT), bf),
            pltpu.VMEM((RV, DV), bf),
            pltpu.VMEM((RT, DT), bf),
            pltpu.VMEM((RV, DV), bf),
            pltpu.VMEM((DV, DV), bf),
            pltpu.VMEM((RT, 2 * CT), bf),
            pltpu.VMEM((RV, 512), bf),
            pltpu.VMEM((RT, 2 * CT), bf),
            pltpu.VMEM((RV, 512), bf),
            dma((2, 4, PARTS)),
            dma((2, 4, 1)),
            dma((1, 4, CHUNKS)),
            dma((1, 4, CHUNKS_V)),
            dma((5,)),
            dma((4,)),
            dma((MB, DT // CT)),
            dma((MB,)),
            dma((2,)),
            dma((2,)),
            dma((2,)),
            dma((DT // CT,)),
            dma((DV // 256,)),
            dma((2,)),
            dma((4,)),
            dma((2, 2, 2)),
            dma((2, 2, 2)),
            pltpu.VMEM((TOK, DT), bf),
            pltpu.VMEM((TOK, DV), bf),
            pltpu.VMEM((RT, DT), f32),
            pltpu.VMEM((RV, DV), f32),
            pltpu.VMEM((TOK, DT), bf),
            pltpu.VMEM((TOK, DV), bf),
            dma((2,)),
            dma((4,)),
        ],
        compiler_params=pltpu.CompilerParams(
            collective_id=0, has_side_effects=True, vmem_limit_bytes=60 * 1024 * 1024
        ),
        name="branches",
    )(
        t5_weight[0],
        vit_weight[0],
        t5_saved.reshape(TOK, DT),
        vit_saved.reshape(TOK, DV),
        t5_top_grad.reshape(TOK, DT),
        vit_top_grad.reshape(TOK, DV),
    )
    gv, g5, dv, d5 = pl.pallas_call(
        hand_over,
        out_shape=tuple(jax.ShapeDtypeStruct(a.shape, a.dtype) for a in (gv, g5, dv, d5)),
        in_specs=[hbm] * 4,
        out_specs=[hbm] * 4,
        scratch_shapes=[pltpu.VMEM(a.shape, a.dtype) for a in (gv, g5, dv, d5)] + [dma((4,)), dma((4,))],
        name="hand_over",
    )(gv, g5, dv, d5)
    return (
        gv.reshape(vit_saved.shape),
        g5.reshape(t5_saved.shape),
        dv[None],
        d5[None],
    )


def solution(mesh):
    placed = (
        P("section", "dp", None),
        P("section", "dp", None),
        P("section", None, "dp", None),
        P("section", None, "dp", None),
        P(None, "dp", None),
        P(None, "dp", None),
    )
    return jax.shard_map(
        shards,
        mesh=mesh,
        in_specs=placed,
        out_specs=(
            P("section", None, "dp", None),
            P("section", None, "dp", None),
            P("section", "dp", None),
            P("section", "dp", None),
        ),
        check_vma=False,
    )
```
